512 devices in a mesh: prow: 16 (over y, z_hi, core), pcol: 32 (over x, z_lo).
Axes of the slice: x: 4, y: 4, z: 16 (z_hi: 2, z_lo: 8; z = z_hi * 8 + z_lo), core: 2. Of those that a mesh axis runs over, the one named last changes fastest.
Arguments:
- tiles: bfloat16 [16, 32, 16, 256, 256], P('prow', 'pcol'), may hold values from -6 to 6
- tile_ids: int32 [16, 32, 16], P('prow', 'pcol'), may hold values from 0 to 127, as said below
- counts: int32 [16, 32], P('prow', 'pcol'), may hold values from 1 to 16, as said below
- pivots: int32 [256], replicated, may hold values from 0 to 65535, as said below
- l_inverse: bfloat16 [256, 256], P(None, 'pcol'), may hold values from -1 to 1, as said below
- u_inverse: bfloat16 [256, 256], P('prow'), may hold values from -0.125 to 0.5, as said below
Outputs:
- factored: bfloat16 [16, 32, 16, 256, 256], P('prow', 'pcol')
The draws below stay inside these ranges and needn't reach their ends.
Inputs may be any that keep to these rules, and one draw needn't show every extreme that they name: Live slot s of device (p, q) holds local tile row tile_ids[p, q, s] // 8 and local tile column tile_ids[p, q, s] % 8; live codes of one device are distinct, padded slots hold arbitrary codes. Let R be the tile rows I >= 1 with tile (I, 0) held and C the tile columns J >= 1 with tile (0, J) held. Tile (0, 0) is held; on each prow index R takes the last one to 3 local tile rows, on each pcol index C takes the last one to 3 local tile columns, and both most counts are reached on some index. Every tile whose row is 0 or in R and whose column is 0 or in C is held; no other held tile lies in tile row 0, a tile row of R, or tile column 0. `counts`: some device has 16 live slots. Row r of tile row 0 and row pivots[r] change places; pivots[r] is r or a row of a tile row of R, and the values that differ from their r are distinct. `l_inverse`: lower triangular with unit diagonal. `u_inverse`: upper triangular with a positive diagonal.
All inputs are finite; a program needn't handle non-finite values.
Results may differ from the reference program's by a relative error of at most 0.0056.
Values may be sent and summed in bfloat16 or wider, within the bound.
A program may use at most 64 MiB of HBM per device.

```python
import jax
import jax.numpy as jnp
from jax import lax

TILE_SIDE = 256
LOCAL_ROWS = 16
LOCAL_COLS = 8
TILE_GRID = 256
TILE_SLOTS = 16
LOWER_MOST = 3
UPPER_MOST = 3
N_PROW = 16
N_PCOL = 32


def layout(key):
    base = jax.random.fold_in(key, 17)
    keys = jax.random.split(base, 9)
    prow_count = TILE_GRID // LOCAL_ROWS
    pcol_count = TILE_GRID // LOCAL_COLS
    positions = LOCAL_ROWS * LOCAL_COLS
    lower_count = jax.random.randint(keys[0], (prow_count,), 1, LOWER_MOST + 1)
    lower_count = lower_count.at[jax.random.randint(keys[1], (), 0, prow_count)].set(LOWER_MOST)
    upper_count = jax.random.randint(keys[2], (pcol_count,), 1, UPPER_MOST + 1)
    upper_count = upper_count.at[jax.random.randint(keys[3], (), 0, pcol_count)].set(UPPER_MOST)
    row_local = jnp.arange(LOCAL_ROWS, dtype=jnp.int32)
    col_local = jnp.arange(LOCAL_COLS, dtype=jnp.int32)
    lower_rows = row_local[None, :] >= LOCAL_ROWS - lower_count[:, None]
    upper_cols = col_local[None, :] >= LOCAL_COLS - upper_count[:, None]
    prow_first = (jnp.arange(prow_count)[:, None] == 0) & (row_local[None, :] == 0)
    pcol_first = (jnp.arange(pcol_count)[:, None] == 0) & (col_local[None, :] == 0)
    row_set = lower_rows | prow_first
    col_set = upper_cols | pcol_first
    grid_shape = (prow_count, pcol_count, LOCAL_ROWS, LOCAL_COLS)
    structural = jnp.broadcast_to(row_set[:, None, :, None] & col_set[None, :, None, :], grid_shape)
    free = jnp.broadcast_to((~row_set)[:, None, :, None] & (~pcol_first)[None, :, None, :], grid_shape)
    structural = structural.reshape(prow_count, pcol_count, positions)
    free = free.reshape(prow_count, pcol_count, positions)
    base_count = jnp.sum(structural.astype(jnp.int32), axis=2)
    room = TILE_SLOTS - base_count
    extra = jax.random.randint(keys[4], (prow_count, pcol_count), 0, room + 1)
    full_row = jax.random.randint(keys[5], (), 0, prow_count)
    full_col = jax.random.randint(keys[6], (), 0, pcol_count)
    extra = extra.at[full_row, full_col].set(room[full_row, full_col])
    place = jnp.arange(positions, dtype=jnp.int32)
    noise = jax.random.randint(keys[7], (prow_count, pcol_count, positions), 0, 2 ** 20)
    score = jnp.where(free, noise * positions + place, -1 - place)
    rank = jnp.argsort(jnp.argsort(-score, axis=2), axis=2)
    chosen = free & (rank < extra[:, :, None])
    present = structural | chosen
    noise_two = jax.random.randint(keys[8], (prow_count, pcol_count, positions), 0, 2 ** 20)
    order_score = jnp.where(present, noise_two * positions + place, -1 - place)
    codes = jnp.argsort(-order_score, axis=2)[:, :, :TILE_SLOTS].astype(jnp.int32)
    live_count = (base_count + extra).astype(jnp.int32)
    return (codes, live_count, lower_rows)


def draw_tile_ids(key, part):
    return layout(key)[0]


def draw_counts(key, part):
    return layout(key)[1]


def draw_pivots(key, part):
    lower_rows = layout(key)[2]
    prow_count = TILE_GRID // LOCAL_ROWS
    total_rows = TILE_GRID * TILE_SIDE
    rows = jnp.arange(total_rows, dtype=jnp.int32)
    tile_row = rows // TILE_SIDE
    eligible = lower_rows[tile_row % prow_count, tile_row // prow_count]
    keys = jax.random.split(jax.random.fold_in(key, 29), 2)
    noise = jax.random.randint(keys[0], (total_rows,), 0, 2 ** 14)
    score = jnp.where(eligible, noise * total_rows + rows, -1)
    picked = jnp.argsort(-score)[:TILE_SIDE].astype(jnp.int32)
    stay = jax.random.randint(keys[1], (TILE_SIDE,), 0, 5) == 0
    return jnp.where(stay, jnp.arange(TILE_SIDE, dtype=jnp.int32), picked)


def draw_l_inverse(key, part):
    first = jax.random.fold_in(jax.random.fold_in(key, 41), 0)
    below = jnp.clip(jax.random.normal(first, (TILE_SIDE, TILE_SIDE), jnp.float32), -4.0, 4.0)
    below = below / jnp.sqrt(jnp.float32(TILE_SIDE))
    return (jnp.tril(below, -1) + jnp.eye(TILE_SIDE, dtype=jnp.float32)).astype(jnp.bfloat16)


def draw_u_inverse(key, part):
    first, second = jax.random.split(jax.random.fold_in(key, 53))
    above = jnp.clip(jax.random.normal(first, (TILE_SIDE, TILE_SIDE), jnp.float32), -4.0, 4.0)
    diagonal = jnp.exp(jax.random.uniform(second, (TILE_SIDE,), jnp.float32, jnp.log(0.5), jnp.log(2.0)))
    above = above / jnp.sqrt(jnp.float32(TILE_SIDE))
    upper = jnp.triu(above, 1) + jnp.diag(diagonal)
    return (upper / 8.0).astype(jnp.bfloat16)


def block_levels(rng, extent, cuts, least, top_value):
    level = 1.0
    for dim, blocks in cuts:
        draws = jax.random.uniform(jax.random.fold_in(jax.random.fold_in(rng, 6), dim), (blocks,), jnp.float32, least / len(cuts), top_value / len(cuts))
        level = level * jnp.repeat(jnp.exp(draws), extent[dim] // blocks).reshape((-1,) + (1,) * (len(extent) - 1 - dim))
    return level


def gaussian(key, dims, deviation, most, shards=(), kind=jnp.bfloat16):
    level = block_levels(key, dims, shards, -0.22, 0.18) if shards else 1.0
    array = jax.random.normal(key, dims, jnp.float32) * deviation * level
    return jnp.minimum(jnp.maximum(array, -most), most).astype(kind)


def setup_inputs(seed: int = 0) -> dict:
    key_of = jax.random.split(jax.random.key(seed), 7)
    tiles = gaussian(key_of[0], (N_PROW, N_PCOL, TILE_SLOTS, TILE_SIDE, TILE_SIDE), 1.0, 6.0, ((0, 16), (1, 32)))
    tile_ids = draw_tile_ids(jax.random.fold_in(key_of[6], 71), 0)
    counts = draw_counts(jax.random.fold_in(key_of[6], 71), 0)
    pivots = draw_pivots(jax.random.fold_in(key_of[6], 71), 0)
    l_inverse = draw_l_inverse(jax.random.fold_in(key_of[6], 71), 0)
    u_inverse = draw_u_inverse(jax.random.fold_in(key_of[6], 71), 0)
    return {"tiles": tiles, "tile_ids": tile_ids, "counts": counts, "pivots": pivots, "l_inverse": l_inverse, "u_inverse": u_inverse}


def reference(tiles, tile_ids, counts, pivots, l_inverse, u_inverse):
    side = TILE_SIDE
    total_rows = TILE_GRID * side
    device_total = N_PROW * N_PCOL * TILE_SLOTS
    flat = tiles.reshape(device_total, side, side)
    flat_rows = flat.reshape(device_total * side, side)
    shape = tile_ids.shape
    prow_of = jnp.broadcast_to(jnp.arange(N_PROW, dtype=jnp.int32)[:, None, None], shape).reshape(-1)
    pcol_of = jnp.broadcast_to(jnp.arange(N_PCOL, dtype=jnp.int32)[None, :, None], shape).reshape(-1)
    slot_of = jnp.broadcast_to(jnp.arange(TILE_SLOTS, dtype=jnp.int32)[None, None, :], shape).reshape(-1)
    alive = slot_of < jnp.broadcast_to(counts[:, :, None], shape).reshape(-1)
    codes = tile_ids.reshape(-1)
    glob_row = (prow_of + N_PROW * (codes // LOCAL_COLS)).astype(jnp.int32)
    glob_col = (pcol_of + N_PCOL * (codes % LOCAL_COLS)).astype(jnp.int32)
    table = jnp.full((TILE_GRID, TILE_GRID), -1, jnp.int32)
    table = table.at[jnp.where(alive, glob_row, TILE_GRID), glob_col].set(
        jnp.arange(device_total, dtype=jnp.int32), mode="drop")

    def fetch(slot, row):
        picked = flat_rows[jnp.maximum(slot, 0) * side + row]
        return jnp.where((slot >= 0)[..., None], picked, jnp.zeros_like(picked))

    every_col = jnp.arange(TILE_GRID, dtype=jnp.int32)
    row_range = jnp.arange(side, dtype=jnp.int32)
    new_slots = table[(pivots // side)[None, :], every_col[:, None]]
    new_top = fetch(new_slots, (pivots % side)[None, :])
    old_slots = jnp.broadcast_to(table[0, :][:, None], (TILE_GRID, side))
    old_top = fetch(old_slots, row_range[None, :])
    anchor_top = jnp.full((total_rows,), -1, jnp.int32).at[pivots].set(row_range)

    def primed_tile(tile, trow, tcol):
        anchor = lax.dynamic_slice_in_dim(anchor_top, (trow * side).astype(jnp.int32), side)
        moved = (anchor >= 0) & (trow >= 1)
        from_top = old_top[tcol][jnp.maximum(anchor, 0)]
        swapped = jnp.where(moved[:, None], from_top, tile)
        return jnp.where(trow == 0, new_top[tcol], swapped)

    lower_slot = table[:, 0]
    upper_slot = table[0, :]
    lower_present = (lower_slot >= 0) & (every_col >= 1)
    upper_present = (upper_slot >= 0) & (every_col >= 1)

    def lower_one(index):
        slot = lower_slot[index]
        tile = flat[jnp.maximum(slot, 0)]
        primed = primed_tile(tile, index, jnp.int32(0))
        value = jnp.dot(primed, u_inverse, preferred_element_type=jnp.float32).astype(jnp.bfloat16)
        return jnp.where(lower_present[index], value, jnp.zeros_like(value))

    def upper_one(index):
        value = jnp.dot(l_inverse, new_top[index], preferred_element_type=jnp.float32).astype(jnp.bfloat16)
        return jnp.where(upper_present[index], value, jnp.zeros_like(value))

    lower_panel = lax.map(lower_one, every_col)
    upper_row = lax.map(upper_one, every_col)

    def finish(index):
        tile = flat[index]
        trow = glob_row[index]
        tcol = glob_col[index]
        primed = primed_tile(tile, trow, tcol)

        def updated(unused):
            product = jnp.dot(lower_panel[trow], upper_row[tcol], preferred_element_type=jnp.float32)
            return (primed.astype(jnp.float32) - product).astype(jnp.bfloat16)

        def kept(unused):
            return primed

        interior = lax.cond(lower_present[trow] & upper_present[tcol], updated, kept, 0)
        value = jnp.where(trow == 0, jnp.where(tcol == 0, primed, upper_row[tcol]),
                          jnp.where(tcol == 0, lower_panel[trow], interior))
        return jnp.where(alive[index], value, jnp.zeros_like(value))

    result = lax.map(finish, jnp.arange(device_total, dtype=jnp.int32))
    return result.reshape(tiles.shape)
```

```python
import jax
import jax.numpy as jnp
from jax import lax
from jax.experimental import pallas as pl
from jax.experimental.pallas import tpu as pltpu
from jax.sharding import PartitionSpec as P

MESH = pl.DeviceIdType.MESH
SIDE = 256
SLOTS = 16
ROW0 = 13
COL0 = 5
BF = jnp.bfloat16
F32 = jnp.float32
VM = pltpu.VMEM


def div(a, b):
    return lax.div(a, jnp.int32(b))


def rem(a, b):
    return lax.rem(a, jnp.int32(b))


def prepare_kernel(ids, counts, piv, tiles, newp, oldp, lowp, corner, table):
    p = lax.axis_index("prow")
    q = lax.axis_index("pcol")
    rows = [0, ROW0, ROW0 + 1, ROW0 + 2]
    cols = [COL0, COL0 + 1, COL0 + 2, 0]
    for r in rows:
        for c in cols:
            table[r * 8 + c] = -1
    for s in range(SLOTS):

        @pl.when(s < counts[0, 0])
        def _():
            table[ids[0, 0, s]] = s

    def tile_at(r, c):
        slot = table[r * 8 + c]
        tile = tiles[0, 0, jnp.maximum(slot, 0)]
        return jnp.where(slot >= 0, tile, jnp.zeros_like(tile))

    lane = lax.broadcasted_iota(jnp.int32, (SIDE, SIDE), 1)
    wanted = piv[...]
    hots = [(wanted == (p + 16 * r) * SIDE + lane).astype(BF) for r in rows]

    def new_column(m, c):
        acc = jnp.zeros((SIDE, SIDE), F32)
        for hot, r in zip(hots, rows):
            acc += jnp.dot(hot, tile_at(r, c), preferred_element_type=F32)
        newp[m] = acc.astype(BF)

    def step(m, carry):
        new_column(m, COL0 + m)
        return carry

    lax.fori_loop(0, 3, step, 0)

    @pl.when(q == 0)
    def _():
        new_column(3, 0)
        for k in range(3):
            lowp[k] = tile_at(ROW0 + k, 0)

    @pl.when(p == 0)
    def _():
        for m in range(3):
            oldp[m] = tile_at(0, COL0 + m)

    @pl.when((p == 0) & (q == 0))
    def _():
        corner[...] = tile_at(0, 0)


TREE = [(4, 0), (2, 0), (1, 0), (6, 4), (5, 4), (3, 2), (7, 6)]


def exchange_kernel(
    newp, oldp, lowp, corner, l_part, u_part,
    both, low, obuf, lbuf, ubuf,
    r1, a1, r2, a2, r3, ro1, ssem, rsem, lsem,
):
    p = lax.axis_index("prow")
    q = lax.axis_index("pcol")
    y, h, c = div(p, 4), rem(div(p, 2), 2), rem(p, 2)
    x, z = div(q, 8), rem(q, 8)
    isq0 = q == 0
    isp0 = p == 0
    corner_dev = isq0 & isp0

    def P_(yy, hh, cc):
        return yy * 4 + hh * 2 + cc

    ys = [rem(y + d, 4) for d in (1, 2, 3)]
    xs = [rem(x + d, 4) for d in (1, 2, 3)]
    zs = [rem(z + d, 8) for d in range(1, 8)]
    d_y = [(P_(v, h, c), q) for v in ys]
    d_h = (P_(y, 1 - h, c), q)
    d_c = (P_(y, h, 1 - c), q)
    d_x = [(p, v * 8 + z) for v in xs]
    d_z = [(p, x * 8 + v) for v in zs]

    bar = pltpu.get_barrier_semaphore()
    greet = d_y + [d_h, d_c] + d_x + d_z
    for dev in greet:
        pl.semaphore_signal(bar, inc=1, device_id=dev, device_id_type=MESH)
    pl.semaphore_wait(bar, len(greet))

    pend = []
    counter = [0, 0]

    def when(cond, fn):
        if cond is None:
            fn()
        else:
            pl.when(cond)(fn)

    def sems(n):
        base = counter[1]
        counter[1] += n
        return [rsem.at[base + i] for i in range(n)]

    def send(src, dst, rs, dev, cond=None):
        d = pltpu.make_async_remote_copy(
            src_ref=src, dst_ref=dst, send_sem=ssem.at[counter[0]], recv_sem=rs,
            device_id=dev, device_id_type=MESH)
        counter[0] += 1
        when(cond, d.start)
        pend.append((cond, d))

    def recv(dst, rs, cond=None):
        d = pltpu.make_async_remote_copy(
            src_ref=dst, dst_ref=dst, send_sem=ssem.at[0], recv_sem=rs,
            device_id=d_c, device_id_type=MESH)
        when(cond, d.wait_recv)

    def al(v, n):
        return pl.multiple_of(v, n)

    def rows32(cc, yy):
        return pl.ds(al(cc * 128 + yy * 32, 32), 32)

    def quarter(v):
        return pl.ds(al(v * 64, 64), 64)

    groups = [(0, 3, None), (3, 1, isq0)]
    gather_groups = [(0, 6, None), (6, 1, isq0)]

    s_n1, s_n2, s_n3 = sems(2), sems(6), sems(2)
    s_n4, s_n5 = sems(6), sems(8)
    s_o1, s_o2, s_o3 = sems(1), sems(1), sems(1)
    s_b1, s_b2, s_b3 = sems(3), sems(3), sems(9)
    s_z1, s_zh, s_z2, s_z3, s_z4, s_z5 = sems(1), sems(1), sems(1), sems(1), sems(3), sems(1)
    s_l1, s_l2 = sems(7), sems(3)
    s_u1, s_u2, s_u3 = sems(1), sems(3), sems(1)

    own_l = pltpu.make_async_copy(l_part, lbuf.at[q], lsem.at[0])
    own_u = pltpu.make_async_copy(u_part, ubuf.at[y, h, c], lsem.at[1])
    own_low = pltpu.make_async_copy(lowp, low, lsem.at[2])
    own_o = pltpu.make_async_copy(corner, obuf, lsem.at[3])
    own_old = pltpu.make_async_copy(oldp.at[:, pl.ds(0, 128)], ro1, lsem.at[4])
    own_l.start()
    own_u.start()
    when(corner_dev, own_o.start)
    when(isq0, own_low.start)
    when(isp0, own_old.start)

    for i, (g, n, cond) in enumerate(groups):
        send(newp.at[pl.ds(g, n), pl.ds(al((1 - c) * 128, 128), 128)], r1.at[pl.ds(g, n)], s_n1[i], d_c, cond)
    send(oldp.at[:, pl.ds(128, 128)], ro1, s_o1[0], d_c, isp0)
    when(corner_dev, own_o.wait)
    rootz = (x == 0) & (z == 0) & (h == 0) & (c == 0)
    for i in range(3):
        send(obuf.at[quarter(ys[i])], obuf.at[quarter(ys[i])], s_z1[0], d_y[i], corner_dev)
    send(obuf.at[quarter(y)], obuf.at[quarter(y)], s_zh[0], d_h, corner_dev)
    own_u.wait()
    send(ubuf.at[y, h, c], ubuf.at[y, h, c], s_u1[0], d_h)
    own_l.wait()
    for i in range(7):
        send(lbuf.at[q], lbuf.at[q], s_l1[i], d_z[i])
    when(isq0, own_low.wait)
    for j in range(3):
        for i in range(3):
            send(low.at[j, quarter(xs[i])], low.at[j, quarter(xs[i])], s_b1[j], d_x[i], isq0)

    def low_tree(parent):
        for j in range(3):
            for child, par in TREE:
                if par == parent:
                    send(low.at[j, quarter(x)], low.at[j, quarter(x)], s_b2[j], (p, x * 8 + child),
                         (z == parent) & (x == 0) if parent == 0 else (z == parent))

    low_tree(0)

    for i, (g, n, cond) in enumerate(groups):
        recv(r1.at[pl.ds(g, n)], s_n1[i], cond)
    a1[...] = newp[:, pl.ds(al(c * 128, 128), 128)] + r1[...]
    for d in range(3):
        for i, (g, n, cond) in enumerate(groups):
            send(a1.at[pl.ds(g, n), pl.ds(al(ys[d] * 32, 32), 32)], r2.at[d, pl.ds(g, n)], s_n2[2 * d + i], d_y[d], cond)
    recv(ro1, s_o1[0], p == 1)
    when(isp0, own_old.wait)
    oldroot = (y == 0) & (h == 0)
    for d in range(3):
        send(ro1.at[:, pl.ds(al(ys[d] * 32, 32), 32)], both.at[pl.ds(3, 3), rows32(c, ys[d])], s_o2[0], d_y[d], oldroot)

    @pl.when(oldroot)
    def _():
        both[pl.ds(3, 3), rows32(c, 0)] = ro1[:, pl.ds(0, 32)]

    second = (x > 0) & (z == 0)
    for j in range(3):
        recv(low.at[j, quarter(x)], s_b1[j], second)
        for child, par in TREE:
            if par == 0:
                send(low.at[j, quarter(x)], low.at[j, quarter(x)], s_b2[j], (p, x * 8 + child), second)
    recv(obuf.at[quarter(y)], s_z1[0], rootz & (y > 0))
    send(obuf.at[quarter(y)], obuf.at[quarter(y)], s_zh[0], d_h, rootz & (y > 0))

    for d in range(3):
        for i, (g, n, cond) in enumerate(groups):
            recv(r2.at[d, pl.ds(g, n)], s_n2[2 * d + i], cond)
    a2[...] = a1[:, pl.ds(al(y * 32, 32), 32)] + r2[0] + r2[1] + r2[2]
    for i, (g, n, cond) in enumerate(groups):
        send(a2.at[pl.ds(g, n)], r3.at[pl.ds(g, n)], s_n3[i], d_h, cond)
    recv(both.at[pl.ds(3, 3), rows32(c, y)], s_o2[0], (h == 0) & (y > 0))
    send(both.at[pl.ds(3, 3), rows32(c, y)], both.at[pl.ds(3, 3), rows32(c, y)], s_o3[0], d_h, h == 0)

    ox = (x == 0) & (c == 0)
    recv(obuf.at[quarter(y)], s_zh[0], ox & (z == 0) & (h == 1))

    def corner_tree(parent):
        for child, par in TREE:
            if par == parent:
                send(obuf.at[quarter(y)], obuf.at[quarter(y)], s_z2[0], (p, x * 8 + child), ox & (z == parent))

    corner_tree(0)
    for j in range(3):
        recv(low.at[j, quarter(x)], s_b2[j], z > 0)
    for parent in (4, 2, 6):
        low_tree(parent)

    root_low = (x == 0) & (z == 0)
    for j in range(3):
        for i in range(3):
            send(low.at[j, quarter(x)], low.at[j, quarter(x)], s_b3[3 * j + i], d_x[i],
                 jnp.logical_not((xs[i] == 0) & (z == 0)))

    for i in range(7):
        recv(lbuf.at[q], s_l1[i])
    for i in range(3):
        send(lbuf.at[pl.ds(x * 8, 8)], lbuf.at[pl.ds(x * 8, 8)], s_l2[i], d_x[i])
    recv(ubuf.at[y, h, c], s_u1[0])
    for i in range(3):
        send(ubuf.at[y, :, c], ubuf.at[y, :, c], s_u2[i], d_y[i])

    recv(obuf.at[quarter(y)], s_z2[0], ox & (z > 0))
    for parent in (4, 2, 6):
        corner_tree(parent)
    for i in range(3):
        send(obuf.at[quarter(y)], obuf.at[quarter(y)], s_z3[0], d_x[i], ox)

    for i, (g, n, cond) in enumerate(groups):
        recv(r3.at[pl.ds(g, n)], s_n3[i], cond)
    both[pl.ds(0, 3), rows32(c, y)] = a2[pl.ds(0, 3)] + r3[pl.ds(0, 3)]

    @pl.when(isq0)
    def _():
        both[6, rows32(c, y)] = a2[3] + r3[3]

    recv(both.at[pl.ds(3, 3), rows32(c, y)], s_o3[0], h == 1)
    for d in range(3):
        for i, (g, n, cond) in enumerate(gather_groups):
            send(both.at[pl.ds(g, n), rows32(c, y)], both.at[pl.ds(g, n), rows32(c, y)], s_n4[2 * d + i], d_y[d], cond)
    for i, (g, n, cond) in enumerate(gather_groups):
        send(both.at[pl.ds(g, n), rows32(c, y)], both.at[pl.ds(g, n), rows32(c, y)], s_n5[i], d_c, cond)
    recv(obuf.at[quarter(y)], s_z3[0], (x > 0) & (c == 0))
    for i in range(3):
        send(obuf.at[quarter(y)], obuf.at[quarter(y)], s_z4[i], d_y[i],
             (c == 0) & jnp.logical_not(isq0 & (ys[i] == 0) & (h == 0)))
    for d in range(3):
        src = rem(y + 3 - d, 4)
        for i, (g, n, cond) in enumerate(gather_groups):
            recv(both.at[pl.ds(g, n), rows32(c, src)], s_n4[2 * d + i], cond)
            send(both.at[pl.ds(g, n), rows32(c, src)], both.at[pl.ds(g, n), rows32(c, src)],
                 s_n5[2 * (d + 1) + i], d_c, cond)
    for i in range(3):
        recv(obuf.at[quarter(rem(y + 3 - i, 4))], s_z4[i], (c == 0) & jnp.logical_not(corner_dev))
    send(obuf, obuf, s_z5[0], d_c, c == 0)
    for i in range(3):
        recv(ubuf.at[rem(y + 3 - i, 4), :, c], s_u2[i])
    send(ubuf.at[:, :, c], ubuf.at[:, :, c], s_u3[0], d_c)

    for j in range(3):
        for i in range(3):
            recv(low.at[j, quarter(rem(x + 3 - i, 4))], s_b3[3 * j + i], jnp.logical_not(root_low))
    for i in range(3):
        recv(lbuf.at[pl.ds(rem(x + 3 - i, 4) * 8, 8)], s_l2[i])
    recv(obuf, s_z5[0], c == 1)
    recv(ubuf.at[:, :, 1 - c], s_u3[0])
    for d in range(4):
        src = rem(y + 4 - d, 4)
        for i, (g, n, cond) in enumerate(gather_groups):
            recv(both.at[pl.ds(g, n), rows32(1 - c, src)], s_n5[2 * d + i], cond)
    for cond, d in pend:
        when(cond, d.wait_send)


def finish_kernel(ids, counts, piv, both, low, corner, l_t, u_inv, tiles, out, lower, upper):
    p = lax.axis_index("prow")
    q = lax.axis_index("pcol")
    block = pl.program_id(0)
    sub = lax.broadcasted_iota(jnp.int32, (SIDE, SIDE), 0)

    def hot_of(row):
        return piv[...] == (p + 16 * row) * SIDE + sub

    def swap(tile, row, old):
        hot = hot_of(row)
        moved = jnp.max(hot.astype(F32), axis=1, keepdims=True) > 0.5
        moved_rows = jnp.dot(hot.astype(BF), old, preferred_element_type=F32)
        return jnp.where(moved, moved_rows, tile.astype(F32))

    @pl.when(block == 0)
    def _():
        lt = l_t[...].astype(F32).reshape(SIDE, SIDE).astype(BF)
        u = u_inv[...].reshape(SIDE, SIDE)

        def step(k, carry):
            s = swap(low[k], ROW0 + k, corner[...]).astype(BF)
            lower[k] = jnp.dot(s, u, preferred_element_type=F32).astype(BF)
            upper[k] = lax.dot_general(
                lt, both[k], (((0,), (0,)), ((), ())), preferred_element_type=F32
            ).astype(BF)
            return carry

        lax.fori_loop(0, 3, step, 0)

    def slot_step(i, carry):
        s = block * 4 + i
        code = ids[0, 0, s]
        row, col = div(code, 8), rem(code, 8)
        live = s < counts[0, 0]
        low_row = row >= ROW0
        up_col = col >= COL0
        k = jnp.maximum(row - ROW0, 0)
        m = jnp.maximum(col - COL0, 0)
        trail = live & low_row & up_col
        top = live & (p == 0) & (row == 0) & up_col
        first = live & (q == 0) & (col == 0) & low_row
        diag = live & (p == 0) & (q == 0) & (code == 0)
        plain = live & jnp.logical_not(trail | top | first | diag)

        @pl.when(trail)
        def _():
            product = jnp.dot(lower[k], upper[m], preferred_element_type=F32)
            out[0, 0, i] = (swap(tiles[0, 0, i], row, both[3 + m]) - product).astype(BF)

        @pl.when(top)
        def _():
            out[0, 0, i] = upper[m]

        @pl.when(first)
        def _():
            out[0, 0, i] = lower[k]

        @pl.when(diag)
        def _():
            out[0, 0, i] = both[6]

        @pl.when(plain)
        def _():
            out[0, 0, i] = tiles[0, 0, i]

        @pl.when(jnp.logical_not(live))
        def _():
            out[0, 0, i] = jnp.zeros((SIDE, SIDE), BF)

        return carry

    lax.fori_loop(0, 4, slot_step, 0)


def body(tiles, tile_ids, counts, pivots, l_inverse, u_inverse):
    tile = (SIDE, SIDE)
    sds = jax.ShapeDtypeStruct
    vmem = pl.BlockSpec(memory_space=VM)
    smem = pl.BlockSpec(memory_space=pltpu.SMEM)
    newp, oldp, lowp, corner = pl.pallas_call(
        prepare_kernel,
        out_shape=(sds((4, *tile), BF), sds((3, *tile), BF), sds((3, *tile), BF), sds(tile, BF)),
        in_specs=[smem, smem, vmem, vmem],
        out_specs=(vmem,) * 4,
        scratch_shapes=[pltpu.SMEM((128,), jnp.int32)],
        name="prepare",
    )(tile_ids, counts, pivots.reshape(SIDE, 1), tiles)
    l_part = l_inverse.T
    dma = pltpu.SemaphoreType.DMA
    both, low, obuf, lbuf, ubuf = pl.pallas_call(
        exchange_kernel,
        out_shape=(
            sds((7, *tile), BF), sds((3, *tile), BF), sds(tile, BF),
            sds((32, 8, SIDE), BF), sds((4, 2, 2, 16, SIDE), BF),
        ),
        in_specs=[vmem] * 6,
        out_specs=(vmem,) * 5,
        scratch_shapes=[
            VM((4, 128, SIDE), BF), VM((4, 128, SIDE), BF), VM((3, 4, 32, SIDE), BF),
            VM((4, 32, SIDE), BF), VM((4, 32, SIDE), BF), VM((3, 128, SIDE), BF),
            dma((160,)), dma((80,)), dma((5,)),
        ],
        compiler_params=pltpu.CompilerParams(collective_id=0, has_side_effects=True),
        name="exchange",
    )(newp, oldp, lowp, corner, l_part, u_inverse)
    whole = lambda *shape: pl.BlockSpec(shape, lambda i: (0,) * len(shape), memory_space=VM)
    return pl.pallas_call(
        finish_kernel,
        grid=(4,),
        out_shape=sds((1, 1, SLOTS, *tile), BF),
        in_specs=[
            smem, smem, whole(1, SIDE), whole(7, *tile), whole(3, *tile), whole(*tile),
            whole(32, 8, SIDE), whole(16, 16, SIDE),
            pl.BlockSpec((1, 1, 4, *tile), lambda i: (0, 0, i, 0, 0), memory_space=VM),
        ],
        out_specs=pl.BlockSpec((1, 1, 4, *tile), lambda i: (0, 0, i, 0, 0), memory_space=VM),
        scratch_shapes=[VM((3, *tile), BF), VM((3, *tile), BF)],
        name="finish",
    )(tile_ids, counts, pivots.reshape(1, SIDE), both, low, obuf, lbuf, ubuf.reshape(16, 16, SIDE), tiles)


def solution(mesh):
    return jax.shard_map(
        body,
        mesh=mesh,
        in_specs=(
            P("prow", "pcol", None, None, None), P("prow", "pcol", None), P("prow", "pcol"),
            P(), P(None, "pcol"), P("prow", None),
        ),
        out_specs=P("prow", "pcol", None, None, None),
        check_vma=False,
    )
```

```python
import jax
import jax.numpy as jnp
from jax import lax
from jax.experimental import pallas as pl
from jax.experimental.pallas import tpu as pltpu
from jax.sharding import PartitionSpec as P

MESH = pl.DeviceIdType.MESH
SIDE = 256
SLOTS = 16
ROW0 = 13
COL0 = 5
BF = jnp.bfloat16
F32 = jnp.float32
VM = pltpu.VMEM


def div(a, b):
    return lax.div(a, jnp.int32(b))


def rem(a, b):
    return lax.rem(a, jnp.int32(b))


TREE = [(4, 0), (2, 0), (1, 0), (6, 4), (5, 4), (3, 2), (7, 6)]
ROWS = (0, ROW0, ROW0 + 1, ROW0 + 2)
COLS = (COL0, COL0 + 1, COL0 + 2, 0)


def exchange_kernel(
    ids, counts, piv, tiles_hbm, l_part, u_part,
    both, low, obuf, lbuf, ubuf,
    tiles, newp, oldp, r1, a1, r2, a2, r3, ro1, ssem, rsem, lsem,
):
    p = lax.axis_index("prow")
    q = lax.axis_index("pcol")
    y, h, c = div(p, 4), rem(div(p, 2), 2), rem(p, 2)
    x, z = div(q, 8), rem(q, 8)
    isq0 = q == 0
    isp0 = p == 0
    corner_dev = isq0 & isp0

    get_tiles = pltpu.make_async_copy(tiles_hbm.at[0, 0], tiles, lsem.at[0])
    get_l = pltpu.make_async_copy(l_part, lbuf.at[q], lsem.at[1])
    get_u = pltpu.make_async_copy(u_part, ubuf.at[y, h, c], lsem.at[2])
    get_tiles.start()
    get_l.start()
    get_u.start()

    def P_(yy, hh, cc):
        return yy * 4 + hh * 2 + cc

    ys = [rem(y + d, 4) for d in (1, 2, 3)]
    xs = [rem(x + d, 4) for d in (1, 2, 3)]
    d_y = [(P_(v, h, c), q) for v in ys]
    d_h = (P_(y, 1 - h, c), q)
    d_c = (P_(y, h, 1 - c), q)
    d_x = [(p, v * 8 + z) for v in xs]
    d_z = [(p, x * 8 + rem(z + d, 8)) for d in range(1, 8)]
    plane = [(rem(y + k // 4, 4), rem(x + k % 4, 4)) for k in range(1, 16)]
    d_plane = [(P_(v, h, c), w * 8 + z) for v, w in plane]
    d_ring = [(P_(y, rem(h + k // 8, 2), c), x * 8 + rem(z + k % 8, 8)) for k in range(1, 16)]

    bar = pltpu.get_barrier_semaphore()
    greet = d_plane + d_ring + [d_c]
    for dev in greet:
        pl.semaphore_signal(bar, inc=1, device_id=dev, device_id_type=MESH)

    def look(s, found):
        code = jnp.where(s < counts[0, 0], ids[0, 0, s], -1)
        return tuple(
            jnp.where(code == ROWS[i // 4] * 8 + COLS[i % 4], s, f) for i, f in enumerate(found)
        )

    slots = lax.fori_loop(0, SLOTS, look, (jnp.int32(-1),) * 16)

    def tile_at(i, j):
        slot = slots[4 * i + j]
        tile = tiles[jnp.maximum(slot, 0)]
        return jnp.where(slot >= 0, tile, jnp.zeros_like(tile))

    sub = lax.broadcasted_iota(jnp.int32, (SIDE, SIDE), 0)
    lane = lax.broadcasted_iota(jnp.int32, (SIDE, SIDE), 1)
    wanted = jnp.sum(jnp.where(sub == lane, piv[...].astype(F32), 0.0), axis=1, keepdims=True)
    hots = [
        (wanted == ((p + 16 * r) * SIDE + lane).astype(F32)).astype(F32).astype(BF) for r in ROWS
    ]
    get_tiles.wait()

    def new_column(m):
        acc = jnp.dot(hots[0], tile_at(0, m), preferred_element_type=F32)
        for i in range(1, 4):
            acc += jnp.dot(hots[i], tile_at(i, m), preferred_element_type=F32)
        newp[m] = acc.astype(BF)

    for m in range(3):
        new_column(m)

    @pl.when(isq0)
    def _():
        new_column(3)
        for k in range(3):
            low[k] = tile_at(1 + k, 3)

    @pl.when(isp0)
    def _():
        for m in range(3):
            old = tile_at(0, m)
            oldp[m] = old
            ro1[m] = old[:128]

    @pl.when(corner_dev)
    def _():
        obuf[...] = tile_at(0, 3).reshape(16, 16, SIDE)

    pl.semaphore_wait(bar, len(greet))

    pend = []
    counter = [0, 0]

    def when(cond, fn):
        if cond is None:
            fn()
        else:
            pl.when(cond)(fn)

    def sems(n):
        base = counter[1]
        counter[1] += n
        return [rsem.at[base + i] for i in range(n)]

    def send(src, dst, rs, dev, cond=None):
        d = pltpu.make_async_remote_copy(
            src_ref=src, dst_ref=dst, send_sem=ssem.at[counter[0]], recv_sem=rs,
            device_id=dev, device_id_type=MESH)
        counter[0] += 1
        when(cond, d.start)
        pend.append((cond, d))

    def recv(dst, rs, cond=None):
        d = pltpu.make_async_remote_copy(
            src_ref=dst, dst_ref=dst, send_sem=ssem.at[0], recv_sem=rs,
            device_id=d_c, device_id_type=MESH)
        when(cond, d.wait_recv)

    def al(v, n):
        return pl.multiple_of(v, n)

    def rows32(cc, yy):
        return pl.ds(al(cc * 128 + yy * 32, 32), 32)

    def quarter(v):
        return pl.ds(al(v * 64, 64), 64)

    groups = [(0, 3, None), (3, 1, isq0)]
    gather_groups = [(0, 6, None), (6, 1, isq0)]

    s_n1, s_n2, s_n3 = sems(2), sems(6), sems(2)
    s_n4, s_n5 = sems(6), sems(8)
    s_o1, s_o2, s_o3 = sems(1), sems(1), sems(1)
    s_b1, s_b2, s_b3 = sems(3), sems(3), sems(9)
    s_c1, s_c2, s_c3, s_c4 = sems(1), sems(1), sems(15), sems(1)
    s_l1, s_l2 = sems(7), sems(3)
    s_u1, s_u2, s_u3 = sems(1), sems(3), sems(1)

    for i, (g, n, cond) in enumerate(groups):
        send(newp.at[pl.ds(g, n), pl.ds(al((1 - c) * 128, 128), 128)], r1.at[pl.ds(g, n)], s_n1[i], d_c, cond)
    send(oldp.at[:, pl.ds(128, 128)], ro1, s_o1[0], d_c, isp0)
    mine = y * 4 + x
    for i, (v, w) in enumerate(plane):
        send(obuf.at[v * 4 + w], obuf.at[v * 4 + w], s_c1[0], d_plane[i], corner_dev)
    source = (z == 0) & (h == 0) & (c == 0)
    for dev in d_ring:
        send(obuf.at[mine], obuf.at[mine], s_c2[0], dev, corner_dev)
    get_u.wait()
    send(ubuf.at[y, h, c], ubuf.at[y, h, c], s_u1[0], d_h)
    get_l.wait()
    for i in range(7):
        send(lbuf.at[q], lbuf.at[q], s_l1[i], d_z[i])
    for j in range(3):
        for i in range(3):
            send(low.at[j, quarter(xs[i])], low.at[j, quarter(xs[i])], s_b1[j], d_x[i], isq0)

    def low_tree(j, parent, cond):
        for child, par in TREE:
            if par == parent:
                send(low.at[j, quarter(x)], low.at[j, quarter(x)], s_b2[j], (p, x * 8 + child), cond)

    def low_ring(j, cond):
        for i in range(3):
            send(low.at[j, quarter(x)], low.at[j, quarter(x)], s_b3[3 * j + i], d_x[i], cond(xs[i]))

    for j in range(3):
        low_tree(j, 0, isq0)

    for i, (g, n, cond) in enumerate(groups):
        recv(r1.at[pl.ds(g, n)], s_n1[i], cond)
    a1[...] = newp[:, pl.ds(al(c * 128, 128), 128)] + r1[...]
    for d in range(3):
        for i, (g, n, cond) in enumerate(groups):
            send(a1.at[pl.ds(g, n), pl.ds(al(ys[d] * 32, 32), 32)], r2.at[d, pl.ds(g, n)], s_n2[2 * d + i], d_y[d], cond)
    recv(ro1, s_o1[0], p == 1)
    oldroot = (y == 0) & (h == 0)
    for d in range(3):
        send(ro1.at[:, pl.ds(al(ys[d] * 32, 32), 32)], both.at[pl.ds(3, 3), rows32(c, ys[d])], s_o2[0], d_y[d], oldroot)

    @pl.when(oldroot)
    def _():
        both[pl.ds(3, 3), rows32(c, 0)] = ro1[:, pl.ds(0, 32)]

    relay = source & jnp.logical_not(corner_dev)
    recv(obuf.at[mine], s_c1[0], relay)
    for dev in d_ring:
        send(obuf.at[mine], obuf.at[mine], s_c2[0], dev, relay)
    second = (x > 0) & (z == 0)
    for j in range(3):
        recv(low.at[j, quarter(x)], s_b1[j], second)
        low_tree(j, 0, second)
    for j in range(3):
        low_ring(j, lambda w: (z == 0) & (w > 0))

    for d in range(3):
        for i, (g, n, cond) in enumerate(groups):
            recv(r2.at[d, pl.ds(g, n)], s_n2[2 * d + i], cond)
    a2[...] = a1[:, pl.ds(al(y * 32, 32), 32)] + r2[0] + r2[1] + r2[2]
    for i, (g, n, cond) in enumerate(groups):
        send(a2.at[pl.ds(g, n)], r3.at[pl.ds(g, n)], s_n3[i], d_h, cond)
    recv(both.at[pl.ds(3, 3), rows32(c, y)], s_o2[0], (h == 0) & (y > 0))
    send(both.at[pl.ds(3, 3), rows32(c, y)], both.at[pl.ds(3, 3), rows32(c, y)], s_o3[0], d_h, h == 0)

    for i in range(7):
        recv(lbuf.at[q], s_l1[i])
    for i in range(3):
        send(lbuf.at[pl.ds(x * 8, 8)], lbuf.at[pl.ds(x * 8, 8)], s_l2[i], d_x[i])
    recv(ubuf.at[y, h, c], s_u1[0])
    for i in range(3):
        send(ubuf.at[y, :, c], ubuf.at[y, :, c], s_u2[i], d_y[i])
    odd = rem(z, 2) == 1
    even = (z > 0) & (rem(z, 2) == 0)
    for j in range(3):
        recv(low.at[j, quarter(x)], s_b2[j], even)
        for parent in (4, 2, 6):
            low_tree(j, parent, z == parent)
    for j in range(3):
        low_ring(j, lambda w: even)

    recv(obuf.at[mine], s_c2[0], (c == 0) & jnp.logical_not(source))
    for i, (v, w) in enumerate(plane):
        send(obuf.at[mine], obuf.at[mine], s_c3[i], d_plane[i],
             (c == 0) & jnp.logical_not((z == 0) & (h == 0) & (v == 0) & (w == 0)))

    for i, (g, n, cond) in enumerate(groups):
        recv(r3.at[pl.ds(g, n)], s_n3[i], cond)
    both[pl.ds(0, 3), rows32(c, y)] = a2[pl.ds(0, 3)] + r3[pl.ds(0, 3)]

    @pl.when(isq0)
    def _():
        both[6, rows32(c, y)] = a2[3] + r3[3]

    recv(both.at[pl.ds(3, 3), rows32(c, y)], s_o3[0], h == 1)
    for d in range(3):
        for i, (g, n, cond) in enumerate(gather_groups):
            send(both.at[pl.ds(g, n), rows32(c, y)], both.at[pl.ds(g, n), rows32(c, y)], s_n4[2 * d + i], d_y[d], cond)
    for i, (g, n, cond) in enumerate(gather_groups):
        send(both.at[pl.ds(g, n), rows32(c, y)], both.at[pl.ds(g, n), rows32(c, y)], s_n5[i], d_c, cond)

    for j in range(3):
        recv(low.at[j, quarter(x)], s_b2[j], odd)
        low_ring(j, lambda w: odd)
    for i in range(3):
        recv(ubuf.at[rem(y + 3 - i, 4), :, c], s_u2[i])
    send(ubuf.at[:, :, c], ubuf.at[:, :, c], s_u3[0], d_c)

    for i, (v, w) in enumerate(plane):
        src = rem(y + 4 - (i + 1) // 4, 4) * 4 + rem(x + 4 - (i + 1) % 4, 4)
        recv(obuf.at[src], s_c3[i], (c == 0) & jnp.logical_not(corner_dev))
    send(obuf, obuf, s_c4[0], d_c, c == 0)
    for d in range(3):
        src = rem(y + 3 - d, 4)
        for i, (g, n, cond) in enumerate(gather_groups):
            recv(both.at[pl.ds(g, n), rows32(c, src)], s_n4[2 * d + i], cond)
            send(both.at[pl.ds(g, n), rows32(c, src)], both.at[pl.ds(g, n), rows32(c, src)],
                 s_n5[2 * (d + 1) + i], d_c, cond)

    for i in range(3):
        recv(lbuf.at[pl.ds(rem(x + 3 - i, 4) * 8, 8)], s_l2[i])
    recv(ubuf.at[:, :, 1 - c], s_u3[0])
    for j in range(3):
        for i in range(3):
            recv(low.at[j, quarter(rem(x + 3 - i, 4))], s_b3[3 * j + i], jnp.logical_not(isq0))
    recv(obuf, s_c4[0], c == 1)
    for d in range(4):
        src = rem(y + 4 - d, 4)
        for i, (g, n, cond) in enumerate(gather_groups):
            recv(both.at[pl.ds(g, n), rows32(1 - c, src)], s_n5[2 * d + i], cond)
    for cond, d in pend:
        when(cond, d.wait_send)


def finish_kernel(ids, counts, piv, both, low, corner, l_t, u_inv, tiles, out, lower, upper):
    p = lax.axis_index("prow")
    q = lax.axis_index("pcol")
    block = pl.program_id(0)
    sub = lax.broadcasted_iota(jnp.int32, (SIDE, SIDE), 0)

    def hot_of(row):
        return piv[...] == (p + 16 * row) * SIDE + sub

    def swap(tile, row, old):
        hot = hot_of(row)
        moved = jnp.max(hot.astype(F32), axis=1, keepdims=True) > 0.5
        moved_rows = jnp.dot(hot.astype(BF), old, preferred_element_type=F32)
        return jnp.where(moved, moved_rows, tile.astype(F32))

    @pl.when(block == 0)
    def _():
        lt = l_t[...].astype(F32).reshape(SIDE, SIDE).astype(BF)
        u = u_inv[...].reshape(SIDE, SIDE)

        def step(k, carry):
            s = swap(low[k], ROW0 + k, corner[...].reshape(SIDE, SIDE)).astype(BF)
            lower[k] = jnp.dot(s, u, preferred_element_type=F32).astype(BF)
            upper[k] = lax.dot_general(
                lt, both[k], (((0,), (0,)), ((), ())), preferred_element_type=F32
            ).astype(BF)
            return carry

        lax.fori_loop(0, 3, step, 0)

    def slot_step(i, carry):
        s = block * 4 + i
        code = ids[0, 0, s]
        row, col = div(code, 8), rem(code, 8)
        live = s < counts[0, 0]
        low_row = row >= ROW0
        up_col = col >= COL0
        k = jnp.maximum(row - ROW0, 0)
        m = jnp.maximum(col - COL0, 0)
        trail = live & low_row & up_col
        top = live & (p == 0) & (row == 0) & up_col
        first = live & (q == 0) & (col == 0) & low_row
        diag = live & (p == 0) & (q == 0) & (code == 0)
        plain = live & jnp.logical_not(trail | top | first | diag)

        @pl.when(trail)
        def _():
            product = jnp.dot(lower[k], upper[m], preferred_element_type=F32)
            out[0, 0, i] = (swap(tiles[0, 0, i], row, both[3 + m]) - product).astype(BF)

        @pl.when(top)
        def _():
            out[0, 0, i] = upper[m]

        @pl.when(first)
        def _():
            out[0, 0, i] = lower[k]

        @pl.when(diag)
        def _():
            out[0, 0, i] = both[6]

        @pl.when(plain)
        def _():
            out[0, 0, i] = tiles[0, 0, i]

        @pl.when(jnp.logical_not(live))
        def _():
            out[0, 0, i] = jnp.zeros((SIDE, SIDE), BF)

        return carry

    lax.fori_loop(0, 4, slot_step, 0)


def body(tiles, tile_ids, counts, pivots, l_inverse, u_inverse):
    tile = (SIDE, SIDE)
    sds = jax.ShapeDtypeStruct
    vmem = pl.BlockSpec(memory_space=VM)
    smem = pl.BlockSpec(memory_space=pltpu.SMEM)
    hbm = pl.BlockSpec(memory_space=pltpu.HBM)
    dma = pltpu.SemaphoreType.DMA
    piv = pivots.reshape(1, SIDE)
    both, low, obuf, lbuf, ubuf = pl.pallas_call(
        exchange_kernel,
        out_shape=(
            sds((7, *tile), BF), sds((3, *tile), BF), sds((16, 16, SIDE), BF),
            sds((32, 8, SIDE), BF), sds((4, 2, 2, 16, SIDE), BF),
        ),
        in_specs=[smem, smem, vmem, hbm, hbm, hbm],
        out_specs=(vmem,) * 5,
        scratch_shapes=[
            VM((SLOTS, *tile), BF), VM((4, *tile), BF), VM((3, *tile), BF),
            VM((4, 128, SIDE), BF), VM((4, 128, SIDE), BF), VM((3, 4, 32, SIDE), BF),
            VM((4, 32, SIDE), BF), VM((4, 32, SIDE), BF), VM((3, 128, SIDE), BF),
            dma((190,)), dma((90,)), dma((3,)),
        ],
        compiler_params=pltpu.CompilerParams(
            collective_id=0, has_side_effects=True, vmem_limit_bytes=24 << 20),
        name="exchange",
    )(tile_ids, counts, piv, tiles, l_inverse.T, u_inverse)
    whole = lambda *shape: pl.BlockSpec(shape, lambda i: (0,) * len(shape), memory_space=VM)
    return pl.pallas_call(
        finish_kernel,
        grid=(4,),
        out_shape=sds((1, 1, SLOTS, *tile), BF),
        in_specs=[
            smem, smem, whole(1, SIDE), whole(7, *tile), whole(3, *tile), whole(16, 16, SIDE),
            whole(32, 8, SIDE), whole(16, 16, SIDE),
            pl.BlockSpec((1, 1, 4, *tile), lambda i: (0, 0, i, 0, 0), memory_space=VM),
        ],
        out_specs=pl.BlockSpec((1, 1, 4, *tile), lambda i: (0, 0, i, 0, 0), memory_space=VM),
        scratch_shapes=[VM((3, *tile), BF), VM((3, *tile), BF)],
        name="finish",
        compiler_params=pltpu.CompilerParams(vmem_limit_bytes=20 << 20),
    )(tile_ids, counts, piv, both, low, obuf, lbuf, ubuf.reshape(16, 16, SIDE), tiles)


def solution(mesh):
    return jax.shard_map(
        body,
        mesh=mesh,
        in_specs=(
            P("prow", "pcol", None, None, None), P("prow", "pcol", None), P("prow", "pcol"),
            P(), P(None, "pcol"), P("prow", None),
        ),
        out_specs=P("prow", "pcol", None, None, None),
        check_vma=False,
    )
```

```python
import jax
import jax.numpy as jnp
from jax import lax
from jax.experimental import pallas as pl
from jax.experimental.pallas import tpu as pltpu
from jax.sharding import PartitionSpec as P

MESH = pl.DeviceIdType.MESH
SIDE = 256
SLOTS = 16
ROW0 = 13
COL0 = 5
BF = jnp.bfloat16
F32 = jnp.float32
VM = pltpu.VMEM
EXCHANGE_VMEM = 24 << 20


def div(a, b):
    return lax.div(a, jnp.int32(b))


def rem(a, b):
    return lax.rem(a, jnp.int32(b))


TREE = [(4, 0), (2, 0), (1, 0), (6, 4), (5, 4), (3, 2), (7, 6)]
ROWS = (0, ROW0, ROW0 + 1, ROW0 + 2)
COLS = (COL0, COL0 + 1, COL0 + 2, 0)


def exchange_kernel(
    ids_hbm, counts, piv_hbm, tiles_hbm, l_part, u_part,
    both, low, obuf, lbuf, ubuf, tiles, piv,
    newp, r1, a1, r2, a2, r3, r4, m4, m5, r5, owner, chips, ids, ssem, rsem, lsem,
):
    p = lax.axis_index("prow")
    q = lax.axis_index("pcol")
    y, h, c = div(p, 4), rem(div(p, 2), 2), rem(p, 2)
    x, z = div(q, 8), rem(q, 8)
    isq0 = q == 0
    isp0 = p == 0
    corner_dev = isq0 & isp0

    get_tiles = pltpu.make_async_copy(tiles_hbm.at[0, 0], tiles, lsem.at[0])
    get_l = pltpu.make_async_copy(l_part, lbuf.at[q], lsem.at[1])
    get_u = pltpu.make_async_copy(u_part, ubuf.at[y, h, c], lsem.at[2])
    get_ids = pltpu.make_async_copy(ids_hbm, ids, lsem.at[3])
    get_piv = pltpu.make_async_copy(piv_hbm, piv, lsem.at[4])
    get_ids.start()
    get_piv.start()
    get_tiles.start()
    get_l.start()
    get_u.start()

    def P_(yy, hh, cc):
        return yy * 4 + hh * 2 + cc

    ys = [rem(y + d, 4) for d in (1, 2, 3)]
    xs = [rem(x + d, 4) for d in (1, 2, 3)]
    d_y = [(P_(v, h, c), q) for v in ys]
    d_h = (P_(y, 1 - h, c), q)
    d_c = (P_(y, h, 1 - c), q)
    d_x = [(p, v * 8 + z) for v in xs]
    d_z = [(p, x * 8 + rem(z + d, 8)) for d in range(1, 8)]
    plane = [(rem(y + k // 4, 4), rem(x + k % 4, 4)) for k in range(1, 16)]
    d_plane = [(P_(v, h, c), w * 8 + z) for v, w in plane]
    d_ring = [(P_(y, rem(h + k // 8, 2), c), x * 8 + rem(z + k % 8, 8)) for k in range(1, 16)]

    bar = pltpu.get_barrier_semaphore()
    greet = d_plane + d_ring + [d_c]
    for dev in greet:
        pl.semaphore_signal(bar, inc=1, device_id=dev, device_id_type=MESH)

    get_ids.wait()

    def look(s, found):
        code = jnp.where(s < counts[0, 0], ids[0, 0, s], -1)
        return tuple(
            jnp.where(code == ROWS[i // 4] * 8 + COLS[i % 4], s, f) for i, f in enumerate(found)
        )

    slots = lax.fori_loop(0, SLOTS, look, (jnp.int32(-1),) * 16)

    def tile_at(i, j):
        slot = slots[4 * i + j]
        tile = tiles[jnp.maximum(slot, 0)]
        return jnp.where(slot >= 0, tile, jnp.zeros_like(tile))

    sub = lax.broadcasted_iota(jnp.int32, (SIDE, SIDE), 0)
    lane = lax.broadcasted_iota(jnp.int32, (SIDE, SIDE), 1)
    get_piv.wait()
    wanted = jnp.sum(jnp.where(sub == lane, piv[...].astype(F32), 0.0), axis=1, keepdims=True)
    trow = jnp.floor(wanted * (1.0 / SIDE))
    holder = trow - 16.0 * jnp.floor(trow * (1.0 / 16))
    chip = jnp.floor(holder * 0.5)
    owner[...] = jnp.broadcast_to(holder, (SIDE, SIDE)).astype(BF)
    chips[...] = jnp.broadcast_to(chip, (SIDE, SIDE)).astype(BF)
    hots = [
        (wanted == ((p + 16 * r) * SIDE + lane).astype(F32)).astype(F32) for r in ROWS
    ]
    given = (isp0 & (holder > 0.5)).astype(F32)
    hots[0] = given * (sub == lane).astype(F32) + (1.0 - given) * hots[0]
    hots = [hot.astype(BF) for hot in hots]
    get_tiles.wait()

    def new_column(m):
        acc = jnp.dot(hots[0], tile_at(0, m), preferred_element_type=F32)
        for i in range(1, 4):
            acc += jnp.dot(hots[i], tile_at(i, m), preferred_element_type=F32)
        newp[m] = acc.astype(BF)

    for m in range(3):
        new_column(m)

    @pl.when(isq0)
    def _():
        new_column(3)
        for k in range(3):
            low[k] = tile_at(1 + k, 3)

    @pl.when(corner_dev)
    def _():
        obuf[...] = tile_at(0, 3).reshape(16, 16, SIDE)

    pl.semaphore_wait(bar, len(greet))

    pend = []
    counter = [0, 0]

    def when(cond, fn):
        if cond is None:
            fn()
        else:
            pl.when(cond)(fn)

    def sems(n):
        base = counter[1]
        counter[1] += n
        return [rsem.at[base + i] for i in range(n)]

    def send(src, dst, rs, dev, cond=None):
        d = pltpu.make_async_remote_copy(
            src_ref=src, dst_ref=dst, send_sem=ssem.at[counter[0]], recv_sem=rs,
            device_id=dev, device_id_type=MESH)
        counter[0] += 1
        when(cond, d.start)
        pend.append((cond, d))

    def recv(dst, rs, cond=None):
        d = pltpu.make_async_remote_copy(
            src_ref=dst, dst_ref=dst, send_sem=ssem.at[0], recv_sem=rs,
            device_id=d_c, device_id_type=MESH)
        when(cond, d.wait_recv)

    def al(v, n):
        return pl.multiple_of(v, n)

    def rows32(cc, yy):
        return pl.ds(al(cc * 128 + yy * 32, 32), 32)

    def quarter(v):
        return pl.ds(al(v * 64, 64), 64)

    s_n1, s_n2, s_n3, s_n4, s_n5 = sems(4), sems(12), sems(4), sems(12), sems(4)
    s_b1, s_b2, s_b3 = sems(3), sems(3), sems(9)
    s_c1, s_c2, s_c3, s_c4 = sems(1), sems(1), sems(15), sems(1)
    s_l1, s_l2 = sems(7), sems(3)
    s_u1, s_u2, s_u3 = sems(1), sems(3), sems(1)
    cols = [(0, None), (1, None), (2, None), (3, isq0)]
    my_half, its_half = pl.ds(al(c * 128, 128), 128), pl.ds(al((1 - c) * 128, 128), 128)
    my_rows = rows32(c, y)
    my_chip = y * 2 + h

    def is_(ref, rows, value):
        return ref[rows] == jnp.full((1, 1), value, F32).astype(BF)

    def run(cond, fn):
        if cond is None:
            fn()
        else:
            pl.when(cond)(fn)

    for m, cond in cols:
        send(newp.at[m, its_half], r1.at[m], s_n1[m], d_c, cond)
    mine = y * 4 + x
    for i, (v, w) in enumerate(plane):
        send(obuf.at[v * 4 + w], obuf.at[v * 4 + w], s_c1[0], d_plane[i], corner_dev)
    source = (z == 0) & (h == 0) & (c == 0)
    for dev in d_ring:
        send(obuf.at[mine], obuf.at[mine], s_c2[0], dev, corner_dev)
    get_u.wait()
    send(ubuf.at[y, h, c], ubuf.at[y, h, c], s_u1[0], d_h)
    get_l.wait()
    for i in range(7):
        send(lbuf.at[q], lbuf.at[q], s_l1[i], d_z[i])
    for j in range(3):
        for i in range(3):
            send(low.at[j, quarter(xs[i])], low.at[j, quarter(xs[i])], s_b1[j], d_x[i], isq0)

    def low_tree(j, parent, cond):
        for child, par in TREE:
            if par == parent:
                send(low.at[j, quarter(x)], low.at[j, quarter(x)], s_b2[j], (p, x * 8 + child), cond)

    def low_ring(j, cond):
        for i in range(3):
            send(low.at[j, quarter(x)], low.at[j, quarter(x)], s_b3[3 * j + i], d_x[i], cond(xs[i]))

    for j in range(3):
        low_tree(j, 0, isq0)

    for m, cond in cols:
        recv(r1.at[m], s_n1[m], cond)

        def chip_rows(m=m):
            own, other = newp[m, my_half], r1[m]
            odd_one = is_(owner, my_half, p + 1 - c)
            keep = jnp.where(c == 0, own, other)
            a1[m] = jnp.where(odd_one, jnp.where(c == 0, other, own), keep)

        run(cond, chip_rows)
        for d in range(3):
            send(a1.at[m, pl.ds(al(ys[d] * 32, 32), 32)], r2.at[m, d], s_n2[3 * m + d], d_y[d], cond)

    relay = source & jnp.logical_not(corner_dev)
    recv(obuf.at[mine], s_c1[0], relay)
    for dev in d_ring:
        send(obuf.at[mine], obuf.at[mine], s_c2[0], dev, relay)
    second = (x > 0) & (z == 0)
    for j in range(3):
        recv(low.at[j, quarter(x)], s_b1[j], second)
        low_tree(j, 0, second)
    for j in range(3):
        low_ring(j, lambda w: (z == 0) & (w > 0))

    for m, cond in cols:
        for d in range(3):
            recv(r2.at[m, d], s_n2[3 * m + d], cond)

        def half_rows(m=m):
            own = a1[m, pl.ds(al(y * 32, 32), 32)]
            got = [r2[m, d] for d in range(3)]
            first = own
            rest = jnp.zeros_like(own)
            for d in range(3):
                at0 = ys[2 - d] == 0
                first = jnp.where(at0, got[d], first)
                rest = rest + jnp.where(at0, own, got[d])
            rest = jnp.where(y == 0, got[0] + got[1] + got[2], rest)
            here = is_(chips, my_rows, 2 + h) | is_(chips, my_rows, 4 + h) | is_(chips, my_rows, 6 + h)
            a2[m, 0] = jnp.where(here, rest, first)
            a2[m, 1] = first

        run(cond, half_rows)
        send(a2.at[m, 0], r3.at[m], s_n3[m], d_h, cond)

    for i in range(7):
        recv(lbuf.at[q], s_l1[i])
    for i in range(3):
        send(lbuf.at[pl.ds(x * 8, 8)], lbuf.at[pl.ds(x * 8, 8)], s_l2[i], d_x[i])
    recv(ubuf.at[y, h, c], s_u1[0])
    for i in range(3):
        send(ubuf.at[y, :, c], ubuf.at[y, :, c], s_u2[i], d_y[i])
    odd = rem(z, 2) == 1
    even = (z > 0) & (rem(z, 2) == 0)
    for j in range(3):
        recv(low.at[j, quarter(x)], s_b2[j], even)
        for parent in (4, 2, 6):
            low_tree(j, parent, z == parent)
    for j in range(3):
        low_ring(j, lambda w: even)

    recv(obuf.at[mine], s_c2[0], (c == 0) & jnp.logical_not(source))
    for i, (v, w) in enumerate(plane):
        send(obuf.at[mine], obuf.at[mine], s_c3[i], d_plane[i],
             (c == 0) & jnp.logical_not((z == 0) & (h == 0) & (v == 0) & (w == 0)))

    for m, cond in cols:
        recv(r3.at[m], s_n3[m], cond)

        def all_rows(m=m):
            mine_, theirs = a2[m, 0], r3[m]
            here = is_(chips, my_rows, h) | is_(chips, my_rows, 2 + h)
            here = here | is_(chips, my_rows, 4 + h) | is_(chips, my_rows, 6 + h)
            new = jnp.where(here, mine_, theirs)
            old = jnp.where(h == 0, a2[m, 1], theirs)
            for d in range(3):
                m4[m, d] = jnp.where(is_(chips, my_rows, ys[d] * 2 + h), old, new)
            r4[m, pl.ds(al(y * 32, 32), 32)] = jnp.where(is_(chips, my_rows, my_chip), old, new)

        run(cond, all_rows)
        for d in range(3):
            send(m4.at[m, d], r4.at[m, pl.ds(al(y * 32, 32), 32)], s_n4[3 * m + d], d_y[d], cond)

    for j in range(3):
        recv(low.at[j, quarter(x)], s_b2[j], odd)
        low_ring(j, lambda w: odd)
    for i in range(3):
        recv(ubuf.at[rem(y + 3 - i, 4), :, c], s_u2[i])
    send(ubuf.at[:, :, c], ubuf.at[:, :, c], s_u3[0], d_c)

    for i, (v, w) in enumerate(plane):
        src = rem(y + 4 - (i + 1) // 4, 4) * 4 + rem(x + 4 - (i + 1) % 4, 4)
        recv(obuf.at[src], s_c3[i], (c == 0) & jnp.logical_not(corner_dev))
    send(obuf, obuf, s_c4[0], d_c, c == 0)
    for m, cond in cols:
        for d in range(3):
            recv(r4.at[m, pl.ds(al(rem(y + 3 - d, 4) * 32, 32), 32)], s_n4[3 * m + d], cond)

        def core_rows(m=m):
            got, chip_ = r4[m], a1[m]
            here = is_(chips, my_half, my_chip)
            new = jnp.where(here, chip_, got)
            own, other = newp[m, my_half], r1[m]
            old = jnp.where(my_chip == 0, jnp.where(c == 0, own, other), got)
            m5[m] = jnp.where(is_(owner, my_half, p + 1 - 2 * c), old, new)
            if m < 3:
                both[m, my_half] = new
                both[3 + m, my_half] = old
            else:
                both[6, my_half] = new

        run(cond, core_rows)
        send(m5.at[m], r5.at[m], s_n5[m], d_c, cond)

    for i in range(3):
        recv(lbuf.at[pl.ds(rem(x + 3 - i, 4) * 8, 8)], s_l2[i])
    recv(ubuf.at[:, :, 1 - c], s_u3[0])
    for j in range(3):
        for i in range(3):
            recv(low.at[j, quarter(rem(x + 3 - i, 4))], s_b3[3 * j + i], jnp.logical_not(isq0))
    recv(obuf, s_c4[0], c == 1)
    for m, cond in cols:
        recv(r5.at[m], s_n5[m], cond)

        def last_rows(m=m):
            got = r5[m]
            new = jnp.where(is_(owner, its_half, p), newp[m, its_half], got)
            if m < 3:
                both[m, its_half] = new
                both[3 + m, its_half] = got
            else:
                both[6, its_half] = new

        run(cond, last_rows)

    @pl.when(isp0)
    def _():
        for m in range(3):
            both[3 + m] = tile_at(0, m)

    for cond, d in pend:
        when(cond, d.wait_send)


def finish_kernel(
    ids_hbm, counts, piv, both, low, corner, l_t, u_inv, tiles, out,
    done, lower, upper, ids, sems,
):
    get_ids = pltpu.make_async_copy(ids_hbm, ids, sems.at[SLOTS])
    get_ids.start()
    p = lax.axis_index("prow")
    q = lax.axis_index("pcol")
    sub = lax.broadcasted_iota(jnp.int32, (SIDE, SIDE), 0)

    def hot_of(row):
        return piv[...] == (p + 16 * row) * SIDE + sub

    def swap(tile, row, old):
        hot = hot_of(row)
        moved = jnp.max(hot.astype(F32), axis=1, keepdims=True) > 0.5
        moved_rows = jnp.dot(hot.astype(BF), old, preferred_element_type=F32)
        return jnp.where(moved, moved_rows, tile.astype(F32))

    def kind(s):
        code = ids[0, 0, s]
        row, col = div(code, 8), rem(code, 8)
        live = s < counts[0, 0]
        low_row = row >= ROW0
        up_col = col >= COL0
        trail = live & low_row & up_col
        top = live & (p == 0) & (row == 0) & up_col
        first = live & (q == 0) & (col == 0) & low_row
        diag = live & (p == 0) & (q == 0) & (code == 0)
        plain = live & jnp.logical_not(trail | top | first | diag)
        k = jnp.maximum(row - ROW0, 0)
        m = jnp.maximum(col - COL0, 0)
        return live, trail, top, first, diag, plain, row, k, m

    def put(src, s):
        return pltpu.make_async_copy(src.at[s], out.at[0, 0, s], sems.at[s])

    def untouched(s, carry):
        live, trail, top, first, diag, plain, row, k, m = kind(s)

        @pl.when(plain)
        def _():
            put(tiles, s).start()

        @pl.when(jnp.logical_not(live))
        def _():
            done[s] = jnp.zeros((SIDE, SIDE), BF)
            put(done, s).start()

        return carry

    lt = l_t[...].astype(F32).reshape(SIDE, SIDE).astype(BF)
    u = u_inv[...].reshape(SIDE, SIDE)

    def solve(k, carry):
        s = swap(low[k], ROW0 + k, corner[...].reshape(SIDE, SIDE)).astype(BF)
        lower[k] = jnp.dot(s, u, preferred_element_type=F32).astype(BF)
        upper[k] = lax.dot_general(
            lt, both[k], (((0,), (0,)), ((), ())), preferred_element_type=F32
        ).astype(BF)
        return carry

    solve(0, 0)
    get_ids.wait()
    lax.fori_loop(0, SLOTS, untouched, 0)
    lax.fori_loop(1, 3, solve, 0)

    def touched(s, carry):
        live, trail, top, first, diag, plain, row, k, m = kind(s)

        @pl.when(trail)
        def _():
            product = jnp.dot(lower[k], upper[m], preferred_element_type=F32)
            done[s] = (swap(tiles[s], row, both[3 + m]) - product).astype(BF)

        @pl.when(top)
        def _():
            done[s] = upper[m]

        @pl.when(first)
        def _():
            done[s] = lower[k]

        @pl.when(diag)
        def _():
            done[s] = both[6]

        @pl.when(trail | top | first | diag)
        def _():
            put(done, s).start()

        return carry

    lax.fori_loop(0, SLOTS, touched, 0)

    def wait(s, carry):
        put(done, s).wait()
        return carry

    lax.fori_loop(0, SLOTS, wait, 0)


def body(tiles, tile_ids, counts, pivots, l_inverse, u_inverse):
    tile = (SIDE, SIDE)
    sds = jax.ShapeDtypeStruct
    vmem = pl.BlockSpec(memory_space=VM)
    smem = pl.BlockSpec(memory_space=pltpu.SMEM)
    hbm = pl.BlockSpec(memory_space=pltpu.HBM)
    dma = pltpu.SemaphoreType.DMA

    def stay(v):
        return pltpu.with_memory_space_constraint(v, pltpu.HBM)

    both, low, obuf, lbuf, ubuf, held, piv = pl.pallas_call(
        exchange_kernel,
        out_shape=(
            sds((7, *tile), BF), sds((3, *tile), BF), sds((16, 16, SIDE), BF),
            sds((32, 8, SIDE), BF), sds((4, 2, 2, 16, SIDE), BF), sds((SLOTS, *tile), BF),
            sds((1, SIDE), jnp.int32),
        ),
        in_specs=[hbm, smem] + [hbm] * 4,
        out_specs=(vmem,) * 7,
        scratch_shapes=[
            VM((4, *tile), BF), VM((4, 128, SIDE), BF), VM((4, 128, SIDE), BF),
            VM((4, 3, 32, SIDE), BF), VM((4, 2, 32, SIDE), BF), VM((4, 32, SIDE), BF),
            VM((4, 128, SIDE), BF), VM((4, 3, 32, SIDE), BF), VM((4, 128, SIDE), BF),
            VM((4, 128, SIDE), BF), VM(tile, BF), VM(tile, BF),
            pltpu.SMEM((1, 1, SLOTS), jnp.int32),
            dma((190,)), dma((90,)), dma((5,)),
        ],
        compiler_params=pltpu.CompilerParams(
            collective_id=0, has_side_effects=True, vmem_limit_bytes=EXCHANGE_VMEM),
        name="exchange",
    )(stay(tile_ids), counts, stay(pivots.reshape(1, SIDE)), stay(tiles), stay(l_inverse.T), stay(u_inverse))
    return pl.pallas_call(
        finish_kernel,
        out_shape=sds((1, 1, SLOTS, *tile), BF),
        in_specs=[hbm, smem] + [vmem] * 7,
        out_specs=hbm,
        scratch_shapes=[
            VM((SLOTS, *tile), BF), VM((3, *tile), BF), VM((3, *tile), BF),
            pltpu.SMEM((1, 1, SLOTS), jnp.int32), dma((SLOTS + 1,)),
        ],
        compiler_params=pltpu.CompilerParams(vmem_limit_bytes=20 << 20),
        name="finish",
    )(stay(tile_ids), counts, piv, both, low, obuf, lbuf, ubuf.reshape(16, 16, SIDE), held)


def solution(mesh):
    return jax.shard_map(
        body,
        mesh=mesh,
        in_specs=(
            P("prow", "pcol", None, None, None), P("prow", "pcol", None), P("prow", "pcol"),
            P(), P(None, "pcol"), P("prow", None),
        ),
        out_specs=P("prow", "pcol", None, None, None),
        check_vma=False,
    )
```

```python
import jax
import jax.numpy as jnp
from jax import lax
from jax.experimental import pallas as pl
from jax.experimental.pallas import tpu as pltpu
from jax.sharding import PartitionSpec as P

MESH = pl.DeviceIdType.MESH
SIDE = 256
SLOTS = 16
ROW0 = 13
COL0 = 5
BF = jnp.bfloat16
F32 = jnp.float32
VM = pltpu.VMEM
EXCHANGE_VMEM = 24 << 20


def div(a, b):
    return lax.div(a, jnp.int32(b))


def rem(a, b):
    return lax.rem(a, jnp.int32(b))


TREE = [(3, 0), (1, 0), (2, 1), (5, 3), (4, 3), (7, 5), (6, 5)]
ROWS = (0, ROW0, ROW0 + 1, ROW0 + 2)
COLS = (COL0, COL0 + 1, COL0 + 2, 0)


def exchange_kernel(
    ids_hbm, counts, piv_hbm, tiles_hbm, l_part, u_part,
    both, low, obuf, lbuf, ubuf, tiles, hot_out, keep_out,
    newp, r1, a1, r2, a2, r3, r4, m4, m5, r5, owner, chips, ids, piv, ssem, rsem, lsem,
):
    p = lax.axis_index("prow")
    q = lax.axis_index("pcol")
    y, h, c = div(p, 4), rem(div(p, 2), 2), rem(p, 2)
    x, z = div(q, 8), rem(q, 8)
    isq0 = q == 0
    isp0 = p == 0
    corner_dev = isq0 & isp0

    get_tiles = pltpu.make_async_copy(tiles_hbm.at[0, 0], tiles, lsem.at[0])
    get_l = pltpu.make_async_copy(l_part, lbuf.at[q], lsem.at[1])
    get_u = pltpu.make_async_copy(u_part, ubuf.at[y, h, c], lsem.at[2])
    get_ids = pltpu.make_async_copy(ids_hbm, ids, lsem.at[3])
    get_piv = pltpu.make_async_copy(piv_hbm, piv, lsem.at[4])
    get_ids.start()
    get_piv.start()
    get_tiles.start()
    get_l.start()
    get_u.start()

    def P_(yy, hh, cc):
        return yy * 4 + hh * 2 + cc

    ys = [rem(y + d, 4) for d in (1, 2, 3)]
    xs = [rem(x + d, 4) for d in (1, 2, 3)]
    d_y = [(P_(v, h, c), q) for v in ys]
    d_h = (P_(y, 1 - h, c), q)
    d_c = (P_(y, h, 1 - c), q)
    d_x = [(p, v * 8 + z) for v in xs]
    d_z = [(p, x * 8 + rem(z + d, 8)) for d in range(1, 8)]
    plane = [(rem(y + k // 4, 4), rem(x + k % 4, 4)) for k in range(1, 16)]
    d_plane = [(P_(v, h, c), w * 8 + z) for v, w in plane]
    d_ring = [(P_(y, rem(h + k // 8, 2), c), x * 8 + rem(z + k % 8, 8)) for k in range(1, 16)]

    bar = pltpu.get_barrier_semaphore()
    greet = d_plane + d_ring + [d_c]
    for dev in greet:
        pl.semaphore_signal(bar, inc=1, device_id=dev, device_id_type=MESH)

    get_ids.wait()

    def look(s, found):
        code = jnp.where(s < counts[0, 0], ids[0, 0, s], -1)
        return tuple(
            jnp.where(code == ROWS[i // 4] * 8 + COLS[i % 4], s, f) for i, f in enumerate(found)
        )

    slots = lax.fori_loop(0, SLOTS, look, (jnp.int32(-1),) * 16)

    def tile_at(i, j):
        slot = slots[4 * i + j]
        tile = tiles[jnp.maximum(slot, 0)]
        return jnp.where(slot >= 0, tile, jnp.zeros_like(tile))

    sub = lax.broadcasted_iota(jnp.int32, (SIDE, SIDE), 0)
    lane = lax.broadcasted_iota(jnp.int32, (SIDE, SIDE), 1)
    get_piv.wait()
    wanted = jnp.sum(jnp.where(sub == lane, piv[...].astype(F32), 0.0), axis=1, keepdims=True)
    trow = jnp.floor(wanted * (1.0 / SIDE))
    holder = trow - 16.0 * jnp.floor(trow * (1.0 / 16))
    chip = jnp.floor(holder * 0.5)
    owner[...] = jnp.broadcast_to(holder, (SIDE, SIDE)).astype(BF)
    chips[...] = jnp.broadcast_to(chip, (SIDE, SIDE)).astype(BF)
    hots = [
        (wanted == ((p + 16 * r) * SIDE + lane).astype(F32)).astype(F32) for r in ROWS
    ]
    given = (isp0 & (holder > 0.5)).astype(F32)
    hots[0] = given * (sub == lane).astype(F32) + (1.0 - given) * hots[0]
    hots = [hot.astype(BF) for hot in hots]
    get_tiles.wait()

    def new_column(m):
        acc = jnp.dot(hots[0], tile_at(0, m), preferred_element_type=F32)
        for i in range(1, 4):
            acc += jnp.dot(hots[i], tile_at(i, m), preferred_element_type=F32)
        newp[m] = acc.astype(BF)

    for m in range(3):
        new_column(m)

    @pl.when(isq0)
    def _():
        new_column(3)
        for k in range(3):
            low[k] = tile_at(1 + k, 3)

    @pl.when(corner_dev)
    def _():
        obuf[...] = tile_at(0, 3).reshape(16, 16, SIDE)

    pl.semaphore_wait(bar, len(greet))

    pend = []
    counter = [0, 0]

    def when(cond, fn):
        if cond is None:
            fn()
        else:
            pl.when(cond)(fn)

    def sems(n):
        base = counter[1]
        counter[1] += n
        return [rsem.at[base + i] for i in range(n)]

    def send(src, dst, rs, dev, cond=None):
        d = pltpu.make_async_remote_copy(
            src_ref=src, dst_ref=dst, send_sem=ssem.at[counter[0]], recv_sem=rs,
            device_id=dev, device_id_type=MESH)
        counter[0] += 1
        when(cond, d.start)
        pend.append((cond, d))

    def recv(dst, rs, cond=None):
        d = pltpu.make_async_remote_copy(
            src_ref=dst, dst_ref=dst, send_sem=ssem.at[0], recv_sem=rs,
            device_id=d_c, device_id_type=MESH)
        when(cond, d.wait_recv)

    def al(v, n):
        return pl.multiple_of(v, n)

    def rows32(cc, yy):
        return pl.ds(al(cc * 128 + yy * 32, 32), 32)

    def quarter(v):
        return pl.ds(al(v * 64, 64), 64)

    s_n1, s_n2, s_n3, s_n4, s_n5 = sems(4), sems(12), sems(4), sems(12), sems(4)
    s_b1, s_b2, s_b3 = sems(3), sems(3), sems(9)
    s_c1, s_c2, s_c3, s_c4 = sems(1), sems(1), sems(15), sems(1)
    s_l1, s_l2 = sems(7), sems(3)
    s_u1, s_u2, s_u3 = sems(1), sems(3), sems(1)
    cols = [(0, None), (1, None), (2, None), (3, isq0)]
    my_half, its_half = pl.ds(al(c * 128, 128), 128), pl.ds(al((1 - c) * 128, 128), 128)
    my_rows = rows32(c, y)
    my_chip = y * 2 + h

    def is_(ref, rows, value):
        return ref[rows] == jnp.full((1, 1), value, F32).astype(BF)

    def run(cond, fn):
        if cond is None:
            fn()
        else:
            pl.when(cond)(fn)

    for m, cond in cols:
        send(newp.at[m, its_half], r1.at[m], s_n1[m], d_c, cond)
    mine = y * 4 + x
    for i, (v, w) in enumerate(plane):
        send(obuf.at[v * 4 + w], obuf.at[v * 4 + w], s_c1[0], d_plane[i], corner_dev)
    source = (z == 0) & (h == 0) & (c == 0)
    for dev in d_ring:
        send(obuf.at[mine], obuf.at[mine], s_c2[0], dev, corner_dev)
    get_u.wait()
    send(ubuf.at[y, h, c], ubuf.at[y, h, c], s_u1[0], d_h)
    get_l.wait()
    for i in range(7):
        send(lbuf.at[q], lbuf.at[q], s_l1[i], d_z[i])
    for j in range(3):
        for i in range(3):
            send(low.at[j, quarter(xs[i])], low.at[j, quarter(xs[i])], s_b1[j], d_x[i], isq0)

    def low_tree(j, parent, cond):
        for child, par in TREE:
            if par == parent:
                send(low.at[j, quarter(x)], low.at[j, quarter(x)], s_b2[j], (p, x * 8 + child), cond)

    def low_ring(j, cond):
        for i in range(3):
            send(low.at[j, quarter(x)], low.at[j, quarter(x)], s_b3[3 * j + i], d_x[i], cond(xs[i]))

    for j in range(3):
        low_tree(j, 0, isq0)

    for k in range(3):
        takes = (piv[...] == (p + 16 * ROWS[k + 1]) * SIDE + sub).astype(F32)
        stays = 1.0 - jnp.max(takes, axis=1, keepdims=True)
        hot_out[k] = takes.astype(BF)
        keep_out[k] = jnp.broadcast_to(stays, (SIDE, SIDE)).astype(BF)

    for m, cond in cols:
        recv(r1.at[m], s_n1[m], cond)

        def chip_rows(m=m):
            own, other = newp[m, my_half], r1[m]
            odd_one = is_(owner, my_half, p + 1 - c)
            keep = jnp.where(c == 0, own, other)
            a1[m] = jnp.where(odd_one, jnp.where(c == 0, other, own), keep)

        run(cond, chip_rows)
        for d in range(3):
            send(a1.at[m, pl.ds(al(ys[d] * 32, 32), 32)], r2.at[m, d], s_n2[3 * m + d], d_y[d], cond)

    relay = source & jnp.logical_not(corner_dev)
    recv(obuf.at[mine], s_c1[0], relay)
    for dev in d_ring:
        send(obuf.at[mine], obuf.at[mine], s_c2[0], dev, relay)
    second = (x > 0) & (z == 0)
    for j in range(3):
        recv(low.at[j, quarter(x)], s_b1[j], second)
        low_tree(j, 0, second)
    for j in range(3):
        low_ring(j, lambda w: (z == 0) & (w > 0))

    for m, cond in cols:
        for d in range(3):
            recv(r2.at[m, d], s_n2[3 * m + d], cond)

        def half_rows(m=m):
            own = a1[m, pl.ds(al(y * 32, 32), 32)]
            got = [r2[m, d] for d in range(3)]
            first = own
            rest = jnp.zeros_like(own)
            for d in range(3):
                at0 = ys[2 - d] == 0
                first = jnp.where(at0, got[d], first)
                rest = rest + jnp.where(at0, own, got[d])
            rest = jnp.where(y == 0, got[0] + got[1] + got[2], rest)
            here = is_(chips, my_rows, 2 + h) | is_(chips, my_rows, 4 + h) | is_(chips, my_rows, 6 + h)
            a2[m, 0] = jnp.where(here, rest, first)
            a2[m, 1] = first

        run(cond, half_rows)
        send(a2.at[m, 0], r3.at[m], s_n3[m], d_h, cond)

    for i in range(7):
        recv(lbuf.at[q], s_l1[i])
    for i in range(3):
        send(lbuf.at[pl.ds(x * 8, 8)], lbuf.at[pl.ds(x * 8, 8)], s_l2[i], d_x[i])
    recv(ubuf.at[y, h, c], s_u1[0])
    for i in range(3):
        send(ubuf.at[y, :, c], ubuf.at[y, :, c], s_u2[i], d_y[i])
    even = (z == 1) | (z == 3) | (z == 5)
    odd = (z > 0) & jnp.logical_not(even)
    for j in range(3):
        recv(low.at[j, quarter(x)], s_b2[j], even)
        for parent in (1, 3, 5):
            low_tree(j, parent, z == parent)
    for j in range(3):
        low_ring(j, lambda w: even)

    recv(obuf.at[mine], s_c2[0], (c == 0) & jnp.logical_not(source))
    for i, (v, w) in enumerate(plane):
        send(obuf.at[mine], obuf.at[mine], s_c3[i], d_plane[i],
             (c == 0) & jnp.logical_not((z == 0) & (h == 0) & (v == 0) & (w == 0)))

    for m, cond in cols:
        recv(r3.at[m], s_n3[m], cond)

        def all_rows(m=m):
            mine_, theirs = a2[m, 0], r3[m]
            here = is_(chips, my_rows, h) | is_(chips, my_rows, 2 + h)
            here = here | is_(chips, my_rows, 4 + h) | is_(chips, my_rows, 6 + h)
            new = jnp.where(here, mine_, theirs)
            old = jnp.where(h == 0, a2[m, 1], theirs)
            for d in range(3):
                m4[m, d] = jnp.where(is_(chips, my_rows, ys[d] * 2 + h), old, new)
            r4[m, pl.ds(al(y * 32, 32), 32)] = jnp.where(is_(chips, my_rows, my_chip), old, new)

        run(cond, all_rows)
        for d in range(3):
            send(m4.at[m, d], r4.at[m, pl.ds(al(y * 32, 32), 32)], s_n4[3 * m + d], d_y[d], cond)

    for j in range(3):
        recv(low.at[j, quarter(x)], s_b2[j], odd)
        low_ring(j, lambda w: odd)
    for i in range(3):
        recv(ubuf.at[rem(y + 3 - i, 4), :, c], s_u2[i])
    send(ubuf.at[:, :, c], ubuf.at[:, :, c], s_u3[0], d_c)

    for i, (v, w) in enumerate(plane):
        src = rem(y + 4 - (i + 1) // 4, 4) * 4 + rem(x + 4 - (i + 1) % 4, 4)
        recv(obuf.at[src], s_c3[i], (c == 0) & jnp.logical_not(corner_dev))
    send(obuf, obuf, s_c4[0], d_c, c == 0)
    for m, cond in cols:
        for d in range(3):
            recv(r4.at[m, pl.ds(al(rem(y + 3 - d, 4) * 32, 32), 32)], s_n4[3 * m + d], cond)

        def core_rows(m=m):
            got, chip_ = r4[m], a1[m]
            here = is_(chips, my_half, my_chip)
            new = jnp.where(here, chip_, got)
            own, other = newp[m, my_half], r1[m]
            old = jnp.where(my_chip == 0, jnp.where(c == 0, own, other), got)
            m5[m] = jnp.where(is_(owner, my_half, p + 1 - 2 * c), old, new)
            if m < 3:
                both[m, my_half] = new
                both[3 + m, my_half] = old
            else:
                both[6, my_half] = new

        run(cond, core_rows)
        send(m5.at[m], r5.at[m], s_n5[m], d_c, cond)

    for i in range(3):
        recv(lbuf.at[pl.ds(rem(x + 3 - i, 4) * 8, 8)], s_l2[i])
    recv(ubuf.at[:, :, 1 - c], s_u3[0])
    for j in range(3):
        for i in range(3):
            recv(low.at[j, quarter(rem(x + 3 - i, 4))], s_b3[3 * j + i], jnp.logical_not(isq0))
    recv(obuf, s_c4[0], c == 1)
    for m, cond in cols:
        recv(r5.at[m], s_n5[m], cond)

        def last_rows(m=m):
            got = r5[m]
            new = jnp.where(is_(owner, its_half, p), newp[m, its_half], got)
            if m < 3:
                both[m, its_half] = new
                both[3 + m, its_half] = got
            else:
                both[6, its_half] = new

        run(cond, last_rows)

    @pl.when(isp0)
    def _():
        for m in range(3):
            both[3 + m] = tile_at(0, m)

    for cond, d in pend:
        when(cond, d.wait_send)


def finish_kernel(
    ids_hbm, counts, hot, keep, both, low, corner, l_t, u_inv, tiles, out,
    done, lower, upper, ids, sems,
):
    get_ids = pltpu.make_async_copy(ids_hbm, ids, sems.at[SLOTS])
    get_ids.start()
    p = lax.axis_index("prow")
    q = lax.axis_index("pcol")

    def swap(tile, k, old):
        moved = jnp.dot(hot[k], old, preferred_element_type=F32)
        return (tile * keep[k]).astype(F32) + moved

    def kind(s):
        code = ids[0, 0, s]
        row, col = div(code, 8), rem(code, 8)
        live = s < counts[0, 0]
        low_row = row >= ROW0
        up_col = col >= COL0
        trail = live & low_row & up_col
        top = live & (p == 0) & (row == 0) & up_col
        first = live & (q == 0) & (col == 0) & low_row
        diag = live & (p == 0) & (q == 0) & (code == 0)
        plain = live & jnp.logical_not(trail | top | first | diag)
        k = jnp.maximum(row - ROW0, 0)
        m = jnp.maximum(col - COL0, 0)
        return live, trail, top, first, diag, plain, row, k, m

    def put(src, s):
        return pltpu.make_async_copy(src.at[s], out.at[0, 0, s], sems.at[s])

    def untouched(s, carry):
        live, trail, top, first, diag, plain, row, k, m = kind(s)

        @pl.when(plain)
        def _():
            put(tiles, s).start()

        @pl.when(jnp.logical_not(live))
        def _():
            done[s] = jnp.zeros((SIDE, SIDE), BF)
            put(done, s).start()

        return carry

    left = jnp.transpose(l_t[...].astype(F32).reshape(SIDE, SIDE)).astype(BF)
    u = u_inv[...].reshape(SIDE, SIDE)

    def solve(k, carry):
        s = swap(low[k], k, corner[...].reshape(SIDE, SIDE)).astype(BF)
        lower[k] = jnp.dot(s, u, preferred_element_type=F32).astype(BF)
        upper[k] = jnp.dot(left, both[k], preferred_element_type=F32).astype(BF)
        return carry

    solve(0, 0)
    get_ids.wait()
    lax.fori_loop(0, SLOTS, untouched, 0)
    lax.fori_loop(1, 3, solve, 0)

    def touched(s, carry):
        live, trail, top, first, diag, plain, row, k, m = kind(s)

        @pl.when(trail)
        def _():
            product = jnp.dot(lower[k], upper[m], preferred_element_type=F32)
            done[s] = (swap(tiles[s], k, both[3 + m]) - product).astype(BF)

        @pl.when(top)
        def _():
            done[s] = upper[m]

        @pl.when(first)
        def _():
            done[s] = lower[k]

        @pl.when(diag)
        def _():
            done[s] = both[6]

        @pl.when(trail | top | first | diag)
        def _():
            put(done, s).start()

        return carry

    lax.fori_loop(0, SLOTS, touched, 0)

    def wait(s, carry):
        put(done, s).wait()
        return carry

    lax.fori_loop(0, SLOTS, wait, 0)


def body(tiles, tile_ids, counts, pivots, l_inverse, u_inverse):
    tile = (SIDE, SIDE)
    sds = jax.ShapeDtypeStruct
    vmem = pl.BlockSpec(memory_space=VM)
    smem = pl.BlockSpec(memory_space=pltpu.SMEM)
    hbm = pl.BlockSpec(memory_space=pltpu.HBM)
    dma = pltpu.SemaphoreType.DMA

    def stay(v):
        return pltpu.with_memory_space_constraint(v, pltpu.HBM)

    both, low, obuf, lbuf, ubuf, held, hot, keep = pl.pallas_call(
        exchange_kernel,
        out_shape=(
            sds((7, *tile), BF), sds((3, *tile), BF), sds((16, 16, SIDE), BF),
            sds((32, 8, SIDE), BF), sds((4, 2, 2, 16, SIDE), BF), sds((SLOTS, *tile), BF),
            sds((3, *tile), BF), sds((3, *tile), BF),
        ),
        in_specs=[hbm, smem] + [hbm] * 4,
        out_specs=(vmem,) * 8,
        scratch_shapes=[
            VM((4, *tile), BF), VM((4, 128, SIDE), BF), VM((4, 128, SIDE), BF),
            VM((4, 3, 32, SIDE), BF), VM((4, 2, 32, SIDE), BF), VM((4, 32, SIDE), BF),
            VM((4, 128, SIDE), BF), VM((4, 3, 32, SIDE), BF), VM((4, 128, SIDE), BF),
            VM((4, 128, SIDE), BF), VM(tile, BF), VM(tile, BF),
            pltpu.SMEM((1, 1, SLOTS), jnp.int32), VM((1, SIDE), jnp.int32),
            dma((190,)), dma((90,)), dma((5,)),
        ],
        compiler_params=pltpu.CompilerParams(
            collective_id=0, has_side_effects=True, vmem_limit_bytes=EXCHANGE_VMEM),
        name="exchange",
    )(stay(tile_ids), counts, stay(pivots.reshape(1, SIDE)), stay(tiles), stay(l_inverse.T), stay(u_inverse))
    return pl.pallas_call(
        finish_kernel,
        out_shape=sds((1, 1, SLOTS, *tile), BF),
        in_specs=[hbm, smem] + [vmem] * 8,
        out_specs=hbm,
        scratch_shapes=[
            VM((SLOTS, *tile), BF), VM((3, *tile), BF), VM((3, *tile), BF),
            pltpu.SMEM((1, 1, SLOTS), jnp.int32), dma((SLOTS + 1,)),
        ],
        compiler_params=pltpu.CompilerParams(vmem_limit_bytes=20 << 20),
        name="finish",
    )(stay(tile_ids), counts, hot, keep, both, low, obuf, lbuf, ubuf.reshape(16, 16, SIDE), held)


def solution(mesh):
    return jax.shard_map(
        body,
        mesh=mesh,
        in_specs=(
            P("prow", "pcol", None, None, None), P("prow", "pcol", None), P("prow", "pcol"),
            P(), P(None, "pcol"), P("prow", None),
        ),
        out_specs=P("prow", "pcol", None, None, None),
        check_vma=False,
    )
```

```python
import jax
import jax.numpy as jnp
from jax import lax
from jax.experimental import pallas as pl
from jax.experimental.pallas import tpu as pltpu
from jax.sharding import PartitionSpec as P

MESH = pl.DeviceIdType.MESH
SIDE = 256
SLOTS = 16
ROW0 = 13
COL0 = 5
BF = jnp.bfloat16
F32 = jnp.float32
VM = pltpu.VMEM
EXCHANGE_VMEM = 24 << 20


def div(a, b):
    return lax.div(a, jnp.int32(b))


def rem(a, b):
    return lax.rem(a, jnp.int32(b))


TREE = [(4, 0), (1, 0), (6, 4), (3, 4), (2, 1), (7, 6), (5, 6)]
ROWS = (0, ROW0, ROW0 + 1, ROW0 + 2)
COLS = (COL0, COL0 + 1, COL0 + 2, 0)


def exchange_kernel(
    ids_hbm, counts, piv_hbm, tiles_hbm, l_part, u_part,
    both, low, obuf, lbuf, ubuf, tiles, hot_out, keep_out,
    newp, r1, a1, r2, a2, r3, r4, m4, m5, r5, owner, chips, ids, piv, ssem, rsem, lsem,
):
    p = lax.axis_index("prow")
    q = lax.axis_index("pcol")
    y, h, c = div(p, 4), rem(div(p, 2), 2), rem(p, 2)
    x, z = div(q, 8), rem(q, 8)
    isq0 = q == 0
    isp0 = p == 0
    corner_dev = isq0 & isp0

    get_tiles = pltpu.make_async_copy(tiles_hbm.at[0, 0], tiles, lsem.at[0])
    get_l = pltpu.make_async_copy(l_part, lbuf.at[q], lsem.at[1])
    get_u = pltpu.make_async_copy(u_part, ubuf.at[y, h, c], lsem.at[2])
    get_ids = pltpu.make_async_copy(ids_hbm, ids, lsem.at[3])
    get_piv = pltpu.make_async_copy(piv_hbm, piv, lsem.at[4])
    get_ids.start()
    get_piv.start()
    get_tiles.start()
    get_l.start()
    get_u.start()

    def P_(yy, hh, cc):
        return yy * 4 + hh * 2 + cc

    ys = [rem(y + d, 4) for d in (1, 2, 3)]
    xs = [rem(x + d, 4) for d in (1, 2, 3)]
    d_y = [(P_(v, h, c), q) for v in ys]
    d_h = (P_(y, 1 - h, c), q)
    d_c = (P_(y, h, 1 - c), q)
    d_x = [(p, v * 8 + z) for v in xs]
    d_z = [(p, x * 8 + rem(z + d, 8)) for d in range(1, 8)]
    plane = [(rem(y + k // 4, 4), rem(x + k % 4, 4)) for k in range(1, 16)]
    d_plane = [(P_(v, h, c), w * 8 + z) for v, w in plane]
    d_ring = [(P_(y, rem(h + k // 8, 2), c), x * 8 + rem(z + k % 8, 8)) for k in range(1, 16)]

    bar = pltpu.get_barrier_semaphore()
    greet = d_plane + d_ring + [d_c]
    for dev in greet:
        pl.semaphore_signal(bar, inc=1, device_id=dev, device_id_type=MESH)

    get_ids.wait()

    def look(s, found):
        code = jnp.where(s < counts[0, 0], ids[0, 0, s], -1)
        return tuple(
            jnp.where(code == ROWS[i // 4] * 8 + COLS[i % 4], s, f) for i, f in enumerate(found)
        )

    slots = lax.fori_loop(0, SLOTS, look, (jnp.int32(-1),) * 16)

    def tile_at(i, j):
        slot = slots[4 * i + j]
        tile = tiles[jnp.maximum(slot, 0)]
        return jnp.where(slot >= 0, tile, jnp.zeros_like(tile))

    sub = lax.broadcasted_iota(jnp.int32, (SIDE, SIDE), 0)
    lane = lax.broadcasted_iota(jnp.int32, (SIDE, SIDE), 1)
    get_piv.wait()
    wanted = jnp.sum(jnp.where(sub == lane, piv[...].astype(F32), 0.0), axis=1, keepdims=True)
    trow = jnp.floor(wanted * (1.0 / SIDE))
    holder = trow - 16.0 * jnp.floor(trow * (1.0 / 16))
    chip = jnp.floor(holder * 0.5)
    owner[...] = jnp.broadcast_to(holder, (SIDE, SIDE)).astype(BF)
    chips[...] = jnp.broadcast_to(chip, (SIDE, SIDE)).astype(BF)
    hots = [
        (wanted == ((p + 16 * r) * SIDE + lane).astype(F32)).astype(F32) for r in ROWS
    ]
    given = (isp0 & (holder > 0.5)).astype(F32)
    hots[0] = given * (sub == lane).astype(F32) + (1.0 - given) * hots[0]
    hots = [hot.astype(BF) for hot in hots]
    get_tiles.wait()

    def new_column(m):
        acc = jnp.dot(hots[0], tile_at(0, m), preferred_element_type=F32)
        for i in range(1, 4):
            acc += jnp.dot(hots[i], tile_at(i, m), preferred_element_type=F32)
        newp[m] = acc.astype(BF)

    for m in range(3):
        new_column(m)

    @pl.when(isq0)
    def _():
        new_column(3)
        for k in range(3):
            low[k] = tile_at(1 + k, 3)

    @pl.when(corner_dev)
    def _():
        obuf[...] = tile_at(0, 3).reshape(16, 16, SIDE)

    pl.semaphore_wait(bar, len(greet))

    pend = []
    counter = [0, 0]

    def when(cond, fn):
        if cond is None:
            fn()
        else:
            pl.when(cond)(fn)

    def sems(n):
        base = counter[1]
        counter[1] += n
        return [rsem.at[base + i] for i in range(n)]

    def send(src, dst, rs, dev, cond=None):
        d = pltpu.make_async_remote_copy(
            src_ref=src, dst_ref=dst, send_sem=ssem.at[counter[0]], recv_sem=rs,
            device_id=dev, device_id_type=MESH)
        counter[0] += 1
        when(cond, d.start)
        pend.append((cond, d))

    def recv(dst, rs, cond=None):
        d = pltpu.make_async_remote_copy(
            src_ref=dst, dst_ref=dst, send_sem=ssem.at[0], recv_sem=rs,
            device_id=d_c, device_id_type=MESH)
        when(cond, d.wait_recv)

    def al(v, n):
        return pl.multiple_of(v, n)

    def rows32(cc, yy):
        return pl.ds(al(cc * 128 + yy * 32, 32), 32)

    def quarter(v):
        return pl.ds(al(v * 64, 64), 64)

    s_n1, s_n2, s_n3, s_n4, s_n5 = sems(4), sems(12), sems(4), sems(12), sems(4)
    s_b1, s_b2, s_b3 = sems(3), sems(3), sems(9)
    s_c1, s_c2, s_c3, s_c4 = sems(1), sems(1), sems(15), sems(1)
    s_l1, s_l2 = sems(7), sems(3)
    s_u1, s_u2, s_u3 = sems(1), sems(3), sems(1)
    cols = [(0, None), (1, None), (2, None), (3, isq0)]
    my_half, its_half = pl.ds(al(c * 128, 128), 128), pl.ds(al((1 - c) * 128, 128), 128)
    my_rows = rows32(c, y)
    my_chip = y * 2 + h

    def is_(ref, rows, value):
        return ref[rows] == jnp.full((1, 1), value, F32).astype(BF)

    def run(cond, fn):
        if cond is None:
            fn()
        else:
            pl.when(cond)(fn)

    for m, cond in cols:
        send(newp.at[m, its_half], r1.at[m], s_n1[m], d_c, cond)
    mine = y * 4 + x
    for i, (v, w) in enumerate(plane):
        send(obuf.at[v * 4 + w], obuf.at[v * 4 + w], s_c1[0], d_plane[i], corner_dev)
    source = (z == 0) & (h == 0) & (c == 0)
    for dev in d_ring:
        send(obuf.at[mine], obuf.at[mine], s_c2[0], dev, corner_dev)
    get_u.wait()
    send(ubuf.at[y, h, c], ubuf.at[y, h, c], s_u1[0], d_h)
    get_l.wait()
    for i in range(7):
        send(lbuf.at[q], lbuf.at[q], s_l1[i], d_z[i])
    for j in range(3):
        for i in range(3):
            send(low.at[j, quarter(xs[i])], low.at[j, quarter(xs[i])], s_b1[j], d_x[i], isq0)

    def low_tree(j, parent, cond):
        for child, par in TREE:
            if par == parent:
                send(low.at[j, quarter(x)], low.at[j, quarter(x)], s_b2[j], (p, x * 8 + child), cond)

    def low_ring(j, cond):
        for i in range(3):
            send(low.at[j, quarter(x)], low.at[j, quarter(x)], s_b3[3 * j + i], d_x[i], cond(xs[i]))

    for j in range(3):
        low_tree(j, 0, isq0)

    for k in range(3):
        takes = (piv[...] == (p + 16 * ROWS[k + 1]) * SIDE + sub).astype(F32)
        stays = 1.0 - jnp.max(takes, axis=1, keepdims=True)
        hot_out[k] = takes.astype(BF)
        keep_out[k] = jnp.broadcast_to(stays, (SIDE, SIDE)).astype(BF)

    for m, cond in cols:
        recv(r1.at[m], s_n1[m], cond)

        def chip_rows(m=m):
            own, other = newp[m, my_half], r1[m]
            odd_one = is_(owner, my_half, p + 1 - c)
            keep = jnp.where(c == 0, own, other)
            a1[m] = jnp.where(odd_one, jnp.where(c == 0, other, own), keep)

        run(cond, chip_rows)
        for d in range(3):
            send(a1.at[m, pl.ds(al(ys[d] * 32, 32), 32)], r2.at[m, d], s_n2[3 * m + d], d_y[d], cond)

    relay = source & jnp.logical_not(corner_dev)
    recv(obuf.at[mine], s_c1[0], relay)
    for dev in d_ring:
        send(obuf.at[mine], obuf.at[mine], s_c2[0], dev, relay)
    second = (x > 0) & (z == 0)
    for j in range(3):
        recv(low.at[j, quarter(x)], s_b1[j], second)
        low_tree(j, 0, second)
    for j in range(3):
        low_ring(j, lambda w: (z == 0) & (w > 0))

    for m, cond in cols:
        for d in range(3):
            recv(r2.at[m, d], s_n2[3 * m + d], cond)

        def half_rows(m=m):
            own = a1[m, pl.ds(al(y * 32, 32), 32)]
            got = [r2[m, d] for d in range(3)]
            first = own
            rest = jnp.zeros_like(own)
            for d in range(3):
                at0 = ys[2 - d] == 0
                first = jnp.where(at0, got[d], first)
                rest = rest + jnp.where(at0, own, got[d])
            rest = jnp.where(y == 0, got[0] + got[1] + got[2], rest)
            here = is_(chips, my_rows, 2 + h) | is_(chips, my_rows, 4 + h) | is_(chips, my_rows, 6 + h)
            a2[m, 0] = jnp.where(here, rest, first)
            a2[m, 1] = first

        run(cond, half_rows)
        send(a2.at[m, 0], r3.at[m], s_n3[m], d_h, cond)

    for i in range(7):
        recv(lbuf.at[q], s_l1[i])
    for i in range(3):
        send(lbuf.at[pl.ds(x * 8, 8)], lbuf.at[pl.ds(x * 8, 8)], s_l2[i], d_x[i])
    recv(ubuf.at[y, h, c], s_u1[0])
    for i in range(3):
        send(ubuf.at[y, :, c], ubuf.at[y, :, c], s_u2[i], d_y[i])
    even = (z == 1) | (z == 4) | (z == 6)
    odd = (z > 0) & jnp.logical_not(even)
    for j in range(3):
        recv(low.at[j, quarter(x)], s_b2[j], even)
        for parent in (1, 4, 6):
            low_tree(j, parent, z == parent)
    for j in range(3):
        low_ring(j, lambda w: even)

    recv(obuf.at[mine], s_c2[0], (c == 0) & jnp.logical_not(source))
    for i, (v, w) in enumerate(plane):
        send(obuf.at[mine], obuf.at[mine], s_c3[i], d_plane[i],
             (c == 0) & jnp.logical_not((z == 0) & (h == 0) & (v == 0) & (w == 0)))

    for m, cond in cols:
        recv(r3.at[m], s_n3[m], cond)

        def all_rows(m=m):
            mine_, theirs = a2[m, 0], r3[m]
            here = is_(chips, my_rows, h) | is_(chips, my_rows, 2 + h)
            here = here | is_(chips, my_rows, 4 + h) | is_(chips, my_rows, 6 + h)
            new = jnp.where(here, mine_, theirs)
            old = jnp.where(h == 0, a2[m, 1], theirs)
            for d in range(3):
                m4[m, d] = jnp.where(is_(chips, my_rows, ys[d] * 2 + h), old, new)
            r4[m, pl.ds(al(y * 32, 32), 32)] = jnp.where(is_(chips, my_rows, my_chip), old, new)

        run(cond, all_rows)
        for d in range(3):
            send(m4.at[m, d], r4.at[m, pl.ds(al(y * 32, 32), 32)], s_n4[3 * m + d], d_y[d], cond)

    for j in range(3):
        recv(low.at[j, quarter(x)], s_b2[j], odd)
        low_ring(j, lambda w: odd)
    for i in range(3):
        recv(ubuf.at[rem(y + 3 - i, 4), :, c], s_u2[i])
    send(ubuf.at[:, :, c], ubuf.at[:, :, c], s_u3[0], d_c)

    for i, (v, w) in enumerate(plane):
        src = rem(y + 4 - (i + 1) // 4, 4) * 4 + rem(x + 4 - (i + 1) % 4, 4)
        recv(obuf.at[src], s_c3[i], (c == 0) & jnp.logical_not(corner_dev))
    send(obuf, obuf, s_c4[0], d_c, c == 0)
    for m, cond in cols:
        for d in range(3):
            recv(r4.at[m, pl.ds(al(rem(y + 3 - d, 4) * 32, 32), 32)], s_n4[3 * m + d], cond)

        def core_rows(m=m):
            got, chip_ = r4[m], a1[m]
            here = is_(chips, my_half, my_chip)
            new = jnp.where(here, chip_, got)
            own, other = newp[m, my_half], r1[m]
            old = jnp.where(my_chip == 0, jnp.where(c == 0, own, other), got)
            m5[m] = jnp.where(is_(owner, my_half, p + 1 - 2 * c), old, new)
            if m < 3:
                both[m, my_half] = new
                both[3 + m, my_half] = old
            else:
                both[6, my_half] = new

        run(cond, core_rows)
        send(m5.at[m], r5.at[m], s_n5[m], d_c, cond)

    for i in range(3):
        recv(lbuf.at[pl.ds(rem(x + 3 - i, 4) * 8, 8)], s_l2[i])
    recv(ubuf.at[:, :, 1 - c], s_u3[0])
    for j in range(3):
        for i in range(3):
            recv(low.at[j, quarter(rem(x + 3 - i, 4))], s_b3[3 * j + i], jnp.logical_not(isq0))
    recv(obuf, s_c4[0], c == 1)
    for m, cond in cols:
        recv(r5.at[m], s_n5[m], cond)

        def last_rows(m=m):
            got = r5[m]
            new = jnp.where(is_(owner, its_half, p), newp[m, its_half], got)
            if m < 3:
                both[m, its_half] = new
                both[3 + m, its_half] = got
            else:
                both[6, its_half] = new

        run(cond, last_rows)

    @pl.when(isp0)
    def _():
        for m in range(3):
            both[3 + m] = tile_at(0, m)

    for cond, d in pend:
        when(cond, d.wait_send)


def finish_kernel(
    ids_hbm, counts, hot, keep, both, low, corner, l_t, u_inv, tiles, out,
    done, lower, upper, ids, sems,
):
    get_ids = pltpu.make_async_copy(ids_hbm, ids, sems.at[SLOTS])
    get_ids.start()
    p = lax.axis_index("prow")
    q = lax.axis_index("pcol")

    def swap(tile, k, old):
        moved = jnp.dot(hot[k], old, preferred_element_type=F32)
        return (tile * keep[k]).astype(F32) + moved

    def kind(s):
        code = ids[0, 0, s]
        row, col = div(code, 8), rem(code, 8)
        live = s < counts[0, 0]
        low_row = row >= ROW0
        up_col = col >= COL0
        trail = live & low_row & up_col
        top = live & (p == 0) & (row == 0) & up_col
        first = live & (q == 0) & (col == 0) & low_row
        diag = live & (p == 0) & (q == 0) & (code == 0)
        plain = live & jnp.logical_not(trail | top | first | diag)
        k = jnp.maximum(row - ROW0, 0)
        m = jnp.maximum(col - COL0, 0)
        return live, trail, top, first, diag, plain, row, k, m

    def put(src, s):
        return pltpu.make_async_copy(src.at[s], out.at[0, 0, s], sems.at[s])

    def untouched(s, carry):
        live, trail, top, first, diag, plain, row, k, m = kind(s)

        @pl.when(plain)
        def _():
            put(tiles, s).start()

        @pl.when(jnp.logical_not(live))
        def _():
            done[s] = jnp.zeros((SIDE, SIDE), BF)
            put(done, s).start()

        return carry

    left = jnp.transpose(l_t[...].astype(F32).reshape(SIDE, SIDE)).astype(BF)
    u = u_inv[...].reshape(SIDE, SIDE)

    def solve(k, carry):
        s = swap(low[k], k, corner[...].reshape(SIDE, SIDE)).astype(BF)
        lower[k] = jnp.dot(s, u, preferred_element_type=F32).astype(BF)
        upper[k] = jnp.dot(left, both[k], preferred_element_type=F32).astype(BF)
        return carry

    solve(0, 0)
    get_ids.wait()
    lax.fori_loop(0, SLOTS, untouched, 0)
    lax.fori_loop(1, 3, solve, 0)

    def touched(s, carry):
        live, trail, top, first, diag, plain, row, k, m = kind(s)

        @pl.when(trail)
        def _():
            product = jnp.dot(lower[k], upper[m], preferred_element_type=F32)
            done[s] = (swap(tiles[s], k, both[3 + m]) - product).astype(BF)

        @pl.when(top)
        def _():
            done[s] = upper[m]

        @pl.when(first)
        def _():
            done[s] = lower[k]

        @pl.when(diag)
        def _():
            done[s] = both[6]

        @pl.when(trail | top | first | diag)
        def _():
            put(done, s).start()

        return carry

    lax.fori_loop(0, SLOTS, touched, 0)

    def wait(s, carry):
        put(done, s).wait()
        return carry

    lax.fori_loop(0, SLOTS, wait, 0)


def body(tiles, tile_ids, counts, pivots, l_inverse, u_inverse):
    tile = (SIDE, SIDE)
    sds = jax.ShapeDtypeStruct
    vmem = pl.BlockSpec(memory_space=VM)
    smem = pl.BlockSpec(memory_space=pltpu.SMEM)
    hbm = pl.BlockSpec(memory_space=pltpu.HBM)
    dma = pltpu.SemaphoreType.DMA

    def stay(v):
        return pltpu.with_memory_space_constraint(v, pltpu.HBM)

    both, low, obuf, lbuf, ubuf, held, hot, keep = pl.pallas_call(
        exchange_kernel,
        out_shape=(
            sds((7, *tile), BF), sds((3, *tile), BF), sds((16, 16, SIDE), BF),
            sds((32, 8, SIDE), BF), sds((4, 2, 2, 16, SIDE), BF), sds((SLOTS, *tile), BF),
            sds((3, *tile), BF), sds((3, *tile), BF),
        ),
        in_specs=[hbm, smem] + [hbm] * 4,
        out_specs=(vmem,) * 8,
        scratch_shapes=[
            VM((4, *tile), BF), VM((4, 128, SIDE), BF), VM((4, 128, SIDE), BF),
            VM((4, 3, 32, SIDE), BF), VM((4, 2, 32, SIDE), BF), VM((4, 32, SIDE), BF),
            VM((4, 128, SIDE), BF), VM((4, 3, 32, SIDE), BF), VM((4, 128, SIDE), BF),
            VM((4, 128, SIDE), BF), VM(tile, BF), VM(tile, BF),
            pltpu.SMEM((1, 1, SLOTS), jnp.int32), VM((1, SIDE), jnp.int32),
            dma((190,)), dma((90,)), dma((5,)),
        ],
        compiler_params=pltpu.CompilerParams(
            collective_id=0, has_side_effects=True, vmem_limit_bytes=EXCHANGE_VMEM),
        name="exchange",
    )(stay(tile_ids), counts, stay(pivots.reshape(1, SIDE)), stay(tiles), stay(l_inverse.T), stay(u_inverse))
    return pl.pallas_call(
        finish_kernel,
        out_shape=sds((1, 1, SLOTS, *tile), BF),
        in_specs=[hbm, smem] + [vmem] * 8,
        out_specs=hbm,
        scratch_shapes=[
            VM((SLOTS, *tile), BF), VM((3, *tile), BF), VM((3, *tile), BF),
            pltpu.SMEM((1, 1, SLOTS), jnp.int32), dma((SLOTS + 1,)),
        ],
        compiler_params=pltpu.CompilerParams(vmem_limit_bytes=20 << 20),
        name="finish",
    )(stay(tile_ids), counts, hot, keep, both, low, obuf, lbuf, ubuf.reshape(16, 16, SIDE), held)


def solution(mesh):
    return jax.shard_map(
        body,
        mesh=mesh,
        in_specs=(
            P("prow", "pcol", None, None, None), P("prow", "pcol", None), P("prow", "pcol"),
            P(), P(None, "pcol"), P("prow", None),
        ),
        out_specs=P("prow", "pcol", None, None, None),
        check_vma=False,
    )
```
